128 devices in a mesh: patch: 16 (over y, z), hidden: 8 (over x, core).
Axes of the slice: x: 4, y: 4, z: 4, core: 2. Of those that a mesh axis runs over, the one named last changes fastest.
Arguments:
- grid_latent: bfloat16 [49152, 512], P('patch'), may hold values from -6 to 6
- mesh_latent: bfloat16 [81920, 512], P('patch'), may hold values from -6 to 6
- edge_latent: bfloat16 [131072, 512], P('patch'), may hold values from -6 to 6
- senders: int32 [131072], P('patch'), may hold values from 0 to 49151, as said below
- receivers: int32 [131072], P('patch'), may hold values from 0 to 81919
- mesh_slot: int32 [81920], replicated, may hold values from 0 to 81919, as said below
- edge_counts: int32 [16], P('patch'), may hold values from 2730 to 8192, as said below
- w_edge: bfloat16 [512, 512], P(None, 'hidden'), may hold values from -0.25 to 0.25
- w_sender: bfloat16 [512, 512], P(None, 'hidden'), may hold values from -0.25 to 0.25
- w_receiver: bfloat16 [512, 512], P(None, 'hidden'), may hold values from -0.25 to 0.25
- edge_bias: float32 [512], P('hidden'), may hold values from -3 to 3
- w_edge_out: bfloat16 [512, 512], P('hidden'), may hold values from -0.25 to 0.25
- edge_out_bias: float32 [512], P('hidden'), may hold values from -3 to 3
- edge_gain: float32 [512], P('hidden'), may hold values from 0.25 to 1.75
- edge_shift: float32 [512], P('hidden'), may hold values from -2 to 2
- w_mesh_in: bfloat16 [512, 512], P(None, 'hidden'), may hold values from -0.25 to 0.25
- w_message_in: bfloat16 [512, 512], P(None, 'hidden'), may hold values from -0.25 to 0.25
- mesh_bias: float32 [512], P('hidden'), may hold values from -3 to 3
- w_mesh_out: bfloat16 [512, 512], P('hidden'), may hold values from -0.25 to 0.25
- mesh_out_bias: float32 [512], P('hidden'), may hold values from -3 to 3
- mesh_gain: float32 [512], P('hidden'), may hold values from 0.25 to 1.75
- mesh_shift: float32 [512], P('hidden'), may hold values from -2 to 2
Outputs:
- mesh_out: bfloat16 [81920, 512], P('patch', 'hidden')
- edge_out: bfloat16 [131072, 512], P('patch', 'hidden')
The draws below stay inside these ranges and needn't reach their ends.
Inputs may be any that keep to these rules, and one draw needn't show every extreme that they name: `mesh_slot`: A permutation of the mesh node ids 0 to 81919; owner block p holds mesh rows p * 5120 to (p + 1) * 5120 - 1. `senders`: edge slots of block p (slots p * 8192 to (p + 1) * 8192 - 1) send from grid nodes p * 3072 to (p + 1) * 3072 - 1. Only the first edge_counts[p] slots of block p are live; some block is full.
All inputs are finite; a program needn't handle non-finite values.
Results may differ from the reference program's by a relative error of at most 0.014.
Values may be sent and summed in bfloat16 or wider, within the bound.
A program may use at most 192 MiB of HBM per device.

```python
import jax
import jax.numpy as jnp
from jax import lax

LATENT = 512
G_DEV = 3072
E_DEV = 8192
MESH_DEV = 5120
GRID = 49152
EDGES = 131072
MESH = 81920
N_HIDDEN = 8


def mesh_order(key):
    return jax.random.permutation(jax.random.fold_in(key, 11), MESH).astype(jnp.int32)


def draw_mesh_slot(key, part):
    return mesh_order(key)


def draw_receivers(key, part):
    order = mesh_order(key)
    inverse = jnp.argsort(order, stable=True).astype(jnp.int32)
    first, second = jax.random.split(jax.random.fold_in(key, 12))
    third = jax.random.fold_in(key, 15)
    position = jnp.arange(EDGES, dtype=jnp.int32)
    blocks = EDGES // E_DEV
    pick = jax.random.randint(first, (EDGES,), 0, 8)
    anywhere = jax.random.randint(third, (EDGES,), 0, blocks).astype(jnp.int32)
    offset = jnp.where(pick == 4, -1, jnp.where(pick == 7, 1, 0)).astype(jnp.int32)
    nearby = (position // E_DEV + offset + blocks) % blocks
    owner = jnp.where(pick < 4, anywhere, nearby).astype(jnp.int32)
    target = owner * MESH_DEV + jax.random.randint(second, (EDGES,), 0, MESH_DEV)
    return jnp.take(inverse, target).astype(jnp.int32)


def draw_senders(key, part):
    position = jnp.arange(EDGES, dtype=jnp.int32)
    local = jax.random.randint(jax.random.fold_in(key, 13), (EDGES,), 0, G_DEV)
    return (position // E_DEV * G_DEV + local).astype(jnp.int32)


def draw_edge_counts(key, part):
    first, second = jax.random.split(jax.random.fold_in(key, 14))
    blocks = EDGES // E_DEV
    counts = jax.random.randint(first, (blocks,), E_DEV // 3, E_DEV + 1)
    fullest = jax.random.randint(second, (), 0, blocks)
    return jnp.where(jnp.arange(blocks) == fullest, E_DEV, counts).astype(jnp.int32)


def steps_of(own_key, extent, shards, smallest, high):
    level, own = 1.0, jax.random.fold_in(own_key, 6)
    for axis_at, shards_of in shards:
        heights = jnp.exp(jax.random.uniform(jax.random.fold_in(own, axis_at), (shards_of,), jnp.float32, smallest / len(shards), high / len(shards)))
        level = level * jnp.repeat(heights, extent[axis_at] // shards_of).reshape([-1 if axis == axis_at else 1 for axis in range(len(extent))])
    return level


def bell_draw(rng, extent, scale, most, shards=(), held_as=jnp.bfloat16):
    entries = scale * jax.random.normal(rng, extent, jnp.float32)
    if shards:
        entries = entries * steps_of(rng, extent, shards, -0.22, 0.18)
    return jnp.clip(entries, -most, most).astype(held_as)


def setup_inputs(seed: int = 0) -> dict:
    key_list = jax.random.split(jax.random.key(seed), 23)
    return {
        "grid_latent": bell_draw(key_list[0], (GRID, LATENT), 1.0, 6.0, ((0, 16),)),
        "mesh_latent": bell_draw(key_list[1], (MESH, LATENT), 1.0, 6.0, ((0, 16),)),
        "edge_latent": bell_draw(key_list[2], (EDGES, LATENT), 1.0, 6.0, ((0, 16),)),
        "senders": draw_senders(jax.random.fold_in(key_list[22], 71), 0),
        "receivers": draw_receivers(jax.random.fold_in(key_list[22], 71), 0),
        "mesh_slot": draw_mesh_slot(jax.random.fold_in(key_list[22], 71), 0),
        "edge_counts": draw_edge_counts(jax.random.fold_in(key_list[22], 71), 0),
        "w_edge": bell_draw(key_list[7], (LATENT, LATENT), LATENT ** -0.5, 0.25, ((1, 8),)),
        "w_sender": bell_draw(key_list[8], (LATENT, LATENT), LATENT ** -0.5, 0.25, ((1, 8),)),
        "w_receiver": bell_draw(key_list[9], (LATENT, LATENT), LATENT ** -0.5, 0.25, ((1, 8),)),
        "edge_bias": bell_draw(key_list[10], (LATENT,), 0.5, 3.0, ((0, 8),), jnp.float32),
        "w_edge_out": bell_draw(key_list[11], (LATENT, LATENT), LATENT ** -0.5, 0.25, ((0, 8),)),
        "edge_out_bias": bell_draw(key_list[12], (LATENT,), 0.5, 3.0, ((0, 8),), jnp.float32),
        "edge_gain": jnp.clip(1.0 + 0.15 * jax.random.normal(key_list[13], (LATENT,), jnp.float32), 0.25, 1.75),
        "edge_shift": bell_draw(key_list[14], (LATENT,), 0.3, 2.0, ((0, 8),), jnp.float32),
        "w_mesh_in": bell_draw(key_list[15], (LATENT, LATENT), LATENT ** -0.5, 0.25, ((1, 8),)),
        "w_message_in": bell_draw(key_list[16], (LATENT, LATENT), LATENT ** -0.5, 0.25, ((1, 8),)),
        "mesh_bias": bell_draw(key_list[17], (LATENT,), 0.5, 3.0, ((0, 8),), jnp.float32),
        "w_mesh_out": bell_draw(key_list[18], (LATENT, LATENT), LATENT ** -0.5, 0.25, ((0, 8),)),
        "mesh_out_bias": bell_draw(key_list[19], (LATENT,), 0.5, 3.0, ((0, 8),), jnp.float32),
        "mesh_gain": jnp.clip(1.0 + 0.15 * jax.random.normal(key_list[20], (LATENT,), jnp.float32), 0.25, 1.75),
        "mesh_shift": bell_draw(key_list[21], (LATENT,), 0.3, 2.0, ((0, 8),), jnp.float32),
    }


def group_sum(hidden_units, w_out):
    width = w_out.shape[0] // N_HIDDEN
    total = jnp.zeros((hidden_units.shape[0], w_out.shape[1]), jnp.float32)
    for group in range(N_HIDDEN):
        part = jnp.dot(hidden_units[:, group * width:(group + 1) * width], w_out[group * width:(group + 1) * width], preferred_element_type=jnp.float32)
        part = lax.optimization_barrier(part.astype(jnp.bfloat16))
        total = total + part.astype(jnp.float32)
    return total

def normalize(values, gain, offset):
    center = lax.optimization_barrier(jnp.mean(values, axis=1, keepdims=True))
    centered = values - center
    spread = lax.optimization_barrier(jnp.mean(centered * centered, axis=1, keepdims=True))
    return centered * lax.rsqrt(spread + 1e-05) * gain + offset

def reference(grid_latent, mesh_latent, edge_latent, senders, receivers, mesh_slot, edge_counts, w_edge, w_sender, w_receiver, edge_bias, w_edge_out, edge_out_bias, edge_gain, edge_shift, w_mesh_in, w_message_in, mesh_bias, w_mesh_out, mesh_out_bias, mesh_gain, mesh_shift):
    target = jnp.take(mesh_slot, receivers).astype(jnp.int32)
    position = jnp.arange(EDGES, dtype=jnp.int32)
    live = (position % E_DEV < jnp.take(edge_counts, position // E_DEV)).astype(jnp.float32)
    receiver_proj = jnp.dot(mesh_latent, w_receiver, preferred_element_type=jnp.float32).astype(jnp.bfloat16)
    sender_proj = jnp.dot(grid_latent, w_sender, preferred_element_type=jnp.float32)
    edge_pre = jnp.dot(edge_latent, w_edge, preferred_element_type=jnp.float32)
    edge_pre = edge_pre + jnp.take(sender_proj, senders, axis=0) + jnp.take(receiver_proj, target, axis=0).astype(jnp.float32) + edge_bias
    edge_hidden = jax.nn.silu(edge_pre).astype(jnp.bfloat16)
    edge_sum = group_sum(edge_hidden, w_edge_out) + edge_out_bias
    message = normalize(edge_sum, edge_gain, edge_shift) * live[:, None]
    edge_out = (edge_latent.astype(jnp.float32) + message).astype(jnp.bfloat16)
    summed = jax.ops.segment_sum(message, target, num_segments=MESH).astype(jnp.bfloat16)
    mesh_pre = jnp.dot(mesh_latent, w_mesh_in, preferred_element_type=jnp.float32) + jnp.dot(summed, w_message_in, preferred_element_type=jnp.float32) + mesh_bias
    mesh_hidden = jax.nn.silu(mesh_pre).astype(jnp.bfloat16)
    mesh_sum = group_sum(mesh_hidden, w_mesh_out) + mesh_out_bias
    mesh_out = (mesh_latent.astype(jnp.float32) + normalize(mesh_sum, mesh_gain, mesh_shift)).astype(jnp.bfloat16)
    return (mesh_out, edge_out)
```

```python
import jax
import jax.numpy as jnp
from jax import lax
from jax.experimental import pallas as pl
from jax.experimental.pallas import tpu as pltpu
from jax.sharding import PartitionSpec as P

EPSILON = 1e-05
F32 = jnp.float32
BF16 = jnp.bfloat16
NP = 16
NH = 8
LAT = 512
GRID = 3072
EDGE = 8192
MESH = 5120
SUB = MESH // NH
BLK = EDGE // NH
LW = LAT // NH
TAB = NP * MESH // 128
C_OWN, C_NEAR, C_FAR = 384, 224, 64
C_BLK = 176
NROW = C_OWN + 2 * C_NEAR + 13 * C_FAR
NCOMP = NH * C_BLK
MCH = 208
DEV = pl.DeviceIdType.MESH


def base_of(s):
    if s == 1:
        return 0
    if s == 15:
        return C_NEAR
    if s == 0:
        return 2 * C_NEAR + 13 * C_FAR
    return 2 * C_NEAR + C_FAR * (s - 2)


def cap_of(s):
    return C_OWN if s == 0 else (C_NEAR if s in (1, 15) else C_FAR)


def iota(shape, dim):
    return lax.broadcasted_iota(jnp.int32, shape, dim).astype(F32)


def dot_nn(a, b):
    return lax.dot_general(a, b, (((1,), (0,)), ((), ())), preferred_element_type=F32)


def dot_nt(a, b):
    return lax.dot_general(a, b, (((1,), (1,)), ((), ())), preferred_element_type=F32)


def onehot(mask):
    return jnp.where(mask, 1.0, 0.0).astype(BF16)


def col_of(row):
    eye = iota((128, 128), 0) == iota((128, 128), 1)
    return jnp.sum(jnp.where(eye, row, 0.0), axis=1, keepdims=True)


def row_of(col):
    eye = iota((128, 128), 0) == iota((128, 128), 1)
    return jnp.sum(jnp.where(eye, col, 0.0), axis=0, keepdims=True)


def norm_rows(values, gain, offset):
    center = jnp.sum(values, axis=1, keepdims=True) * (1.0 / LAT)
    centered = values - center
    spread = jnp.sum(centered * centered, axis=1, keepdims=True) * (1.0 / LAT)
    return centered * lax.rsqrt(spread + EPSILON) * gain + offset


def silu(v):
    return v / (1.0 + jnp.exp(-v))


def kernel(
    recv_i, send_i, slot, cnt, el_hbm, grid_hbm, mesh_hbm,
    w0, w1, w2, w3, w4, w5, w6,
    b0, b1, b2, b3, b4, b5, b6, b7,
    mo_hbm, eo_hbm, flag_ref,
    el, grid, blk, wfull, tb, tbr, oh, s_ref, sub_ref, r_ref, sd_ref, m_ref, rk_ref, o_ref,
    posb, posc, aq, bq, req_acc, req, reqr, mb, m2_ref, posx,
    xcm, metac, xb, pre, srow, soh, serve, recvrows, scoh, msgb, mrecv, eob, pcrow, eoc, recvx,
    mot, eot, summed, vecs, flagr,
    lsem, wlsem, t_ss, t_rs, w_ss, w_rs, f_ss, f_rs, q_ss, q_rs, g_ss, g_rs, m_ss, m_rs,
    x_ss, x_rs, mo_ss, mo_rs, eo_ss, eo_rs, fl_ss, fl_rs,
):
    p = lax.axis_index("patch")
    h = lax.axis_index("hidden")
    hf = h.astype(F32)
    pf = p.astype(F32)

    def hp(d):
        return lax.rem(h + d, NH)

    def pp(s):
        return lax.rem(p + s, NP)

    def remote(src, dst, ss, rs, dev):
        return pltpu.make_async_remote_copy(
            src_ref=src, dst_ref=dst, send_sem=ss, recv_sem=rs, device_id=dev, device_id_type=DEV
        )

    loads = [
        pltpu.make_async_copy(
            mesh_hbm.at[pl.ds(pl.multiple_of(h * SUB, SUB), SUB), :], blk, lsem.at[2]
        ),
        pltpu.make_async_copy(el_hbm, el, lsem.at[0]),
        pltpu.make_async_copy(grid_hbm, grid, lsem.at[1]),
    ]
    wsrc = (w0, w1, w2, w3, w4, w5, w6)
    wl = [pltpu.make_async_copy(wsrc[k], wfull.at[h, k], wlsem.at[k]) for k in range(7)]
    for c in wl:
        c.start()
    for c in loads:
        c.start()
    barrier = pltpu.get_barrier_semaphore()
    for d in range(1, NH):
        pl.semaphore_signal(barrier, inc=1, device_id=(p, hp(d)), device_id_type=DEV)
    for s in range(1, NP):
        pl.semaphore_signal(barrier, inc=1, device_id=(pp(s), h), device_id_type=DEV)

    h8 = pl.multiple_of(h * 8, 8)
    rr = recv_i[pl.ds(h8, 8), :]
    rhi = lax.shift_right_logical(rr, 7).astype(F32)
    rlo = (rr & 127).astype(F32)
    vt = slot[...].astype(F32).T
    va = jnp.floor(vt * (1.0 / 256.0))
    vb = vt - va * 256.0
    i640 = iota((TAB, 128), 0)
    for k in range(8):
        oh[:, 128 * k : 128 * (k + 1)] = onehot(i640 == rhi[k : k + 1, :])
    ohv = oh[...]
    la = dot_nn((va - 256.0).astype(BF16), ohv)
    lb = dot_nn(vb.astype(BF16), ohv)
    i128 = iota((128, 128), 0)
    for k in range(8):
        pick = i128 == rlo[k : k + 1, :]
        both = (la[:, 128 * k : 128 * (k + 1)] + 256.0) * 256.0 + lb[:, 128 * k : 128 * (k + 1)]
        tb[k : k + 1, :] = jnp.sum(jnp.where(pick, both, 0.0), axis=0, keepdims=True)
    for k, b in enumerate((b0, b1, b2, b3, b4, b5, b6, b7)):
        tb[8 + k : 9 + k, 0:LW] = b[...]
        tb[8 + k : 9 + k, LW:128] = b[...]

    pl.semaphore_wait(barrier, NH - 1 + NP - 1)
    t_copies = [
        remote(tb, tbr.at[h], t_ss.at[d], t_rs.at[d], (p, hp(d))) for d in range(1, NH)
    ]
    for c in t_copies:
        c.start()
    tbr[h] = tb[...]
    for c in wl:
        c.wait()
    partner = h + 1 - 2 * lax.rem(h, 2)
    w_copies = []
    for part, (lo, n) in enumerate(((0, 4), (4, 3))):
        for d in (1, 3, 2):
            i = part * 4 + d
            c = remote(
                wfull.at[h, pl.ds(lo, n)], wfull.at[h, pl.ds(lo, n)], w_ss.at[i], w_rs.at[i],
                (p, hp(2 * d)),
            )
            c.start()
            w_copies.append(c)
        c = remote(
            wfull.at[h, pl.ds(lo, n)], wfull.at[h, pl.ds(lo, n)], f_ss.at[part * 4], f_rs.at[part * 4],
            (p, partner),
        )
        c.start()
        w_copies.append(c)

    def from_chip(part, d):
        lo, n = ((0, 4), (4, 3))[part]
        src_h = lax.rem(h + NH - 2 * d, NH)
        ref = wfull.at[src_h, pl.ds(lo, n)]
        i = part * 4 + d
        return (
            remote(ref, ref, w_ss.at[i], w_rs.at[i], (p, hp(2 * d))),
            remote(ref, ref, f_ss.at[i], f_rs.at[i], (p, partner)),
        )

    def forward(part):
        for d in (1, 3, 2):
            arrival, fwd = from_chip(part, d)
            arrival.wait_recv()
            fwd.start()

    def weights_ready(part):
        lo, n = ((0, 4), (4, 3))[part]
        for d in range(4):
            src_h = lax.rem(partner + NH - 2 * d, NH)
            ref = wfull.at[src_h, pl.ds(lo, n)]
            remote(ref, ref, f_ss.at[part * 4 + d], f_rs.at[part * 4 + d], (p, partner)).wait_recv()

    tri = jnp.where(iota((128, 256), 1) < 128.0,
                    jnp.where(iota((128, 256), 0) < iota((128, 256), 1), 1.0, 0.0), 1.0).astype(BF16)
    i16 = iota((16, 128), 0)
    base16 = jnp.where(
        i16 == 0.0, float(base_of(0)),
        jnp.where(i16 == 1.0, 0.0, jnp.where(i16 == 15.0, float(C_NEAR), 2.0 * C_NEAR + C_FAR * (i16 - 2.0))),
    )
    cap16 = jnp.where(i16 == 0.0, float(C_OWN), jnp.where((i16 == 1.0) | (i16 == 15.0), float(C_NEAR), float(C_FAR)))
    i48 = iota((48, 128), 0)

    for c in t_copies:
        c.wait_recv()

    tf = tbr[:, 0:8, :].reshape(64, 128)
    q = jnp.floor((tf + 0.5) * (1.0 / MESH))
    rem = tf - q * MESH
    sub = jnp.floor((rem + 0.5) * (1.0 / SUB))
    r1 = rem - sub * SUB + 1.0
    shift = q - pf
    shift = jnp.where(shift < 0.0, shift + NP, shift)
    eidx = lax.broadcasted_iota(jnp.int32, (64, 128), 0) * 128 + lax.broadcasted_iota(jnp.int32, (64, 128), 1)
    live = eidx < cnt[0]
    own = live & (sub == hf)
    s_ref[...] = jnp.where(own, shift, -1.0)
    sub_ref[...] = jnp.where(live, sub, -1.0)
    r_ref[...] = r1
    sd_ref[...] = (send_i[...] - p * GRID).astype(F32)
    o_ref[...] = dot_nn(onehot(own), tri)

    def mark(b, _):
        st = s_ref[pl.ds(pl.multiple_of(b * 8, 8), 8), :]
        for k in range(8):
            m_ref[pl.ds(pl.multiple_of(b * 128 + 16 * k, 16), 16), :] = onehot(i16 == st[k : k + 1, :])
        return 0

    lax.fori_loop(0, 8, mark, 0)
    rk_ref[...] = dot_nn(m_ref[...], tri)
    req_acc[...] = jnp.zeros_like(req_acc)

    def place(b, carry):
        counts, most = carry
        b8 = pl.ds(pl.multiple_of(b * 8, 8), 8)
        st = s_ref[b8, :]
        rt = r_ref[b8, :]
        ot = o_ref[b8, :]
        rowcount = jnp.zeros((1, 128), F32)
        pbs, pcs = [], []
        vhi = jnp.floor(rt * (1.0 / 256.0))
        vlo = rt - vhi * 256.0
        for k in range(8):
            i0 = pl.ds(pl.multiple_of(b * 128 + 16 * k, 16), 16)
            rk = rk_ref[i0, :]
            mk = m_ref[i0, :].astype(F32)
            rank = rk[:, :128] + counts
            counts = counts + rk[:, 128:]
            isown = st[k : k + 1, :] >= 0.0
            pb = jnp.sum(mk * (base16 + rank), axis=0, keepdims=True)
            rk1 = jnp.sum(mk * rank, axis=0, keepdims=True)
            pbs.append(jnp.where(isown, pb, -1.0))
            pcs.append(jnp.where(isown, ot[k : k + 1, :128] + rowcount, -1.0))
            rowcount = rowcount + ot[k : k + 1, 128:]
            qhi0 = jnp.floor(rk1 * (1.0 / 128.0))
            qlo = rk1 - qhi0 * 128.0
            qhi = jnp.where(isown & (qhi0 < 3.0), st[k : k + 1, :] * 3.0 + qhi0, -1.0)
            hit = i48 == qhi
            lanes = slice(128 * k, 128 * (k + 1))
            aq[0:48, lanes] = jnp.where(hit, vhi[k : k + 1, :], 0.0).astype(BF16)
            aq[48:96, lanes] = jnp.where(hit, vlo[k : k + 1, :], 0.0).astype(BF16)
            bq[:, lanes] = onehot(i128 == qlo)
        for k in range(8):
            posb[pl.ds(b * 8 + k, 1), :] = pbs[k]
            posc[pl.ds(b * 8 + k, 1), :] = pcs[k]
        req_acc[...] += dot_nt(aq[...], bq[...])
        return counts, jnp.maximum(most, rowcount)

    counts, most = lax.fori_loop(0, 8, place, (jnp.zeros((16, 128), F32), jnp.zeros((1, 128), F32)))
    over = jnp.max(jnp.where(counts > cap16, 1.0, 0.0), axis=0, keepdims=True)
    over = jnp.maximum(over, jnp.where(most > float(C_BLK), 1.0, 0.0))
    for s in range(NP):
        req[s, 0:3, :] = req_acc[3 * s : 3 * s + 3, :] * 256.0 + req_acc[48 + 3 * s : 48 + 3 * s + 3, :] - 1.0
        req[s, 3:7, :] = jnp.full((4, 128), -1.0, F32)
        req[s, 7:8, :] = over
    q_copies = [
        remote(req.at[s], reqr.at[s], q_ss.at[s], q_rs.at[s], (pp(s), h)) for s in range(1, NP)
    ]
    for c in q_copies:
        c.start()
    reqr[0] = req[0]

    for c in loads:
        c.wait()
    ic = iota((C_BLK, 128), 0)
    mb[...] = jnp.zeros_like(mb)

    def compact(b, _):
        b8 = pl.ds(pl.multiple_of(b * 8, 8), 8)
        pct = posc[b8, :]
        pbt = posb[b8, :]
        sdt = sd_ref[b8, :]
        phi = jnp.floor(pbt * (1.0 / 128.0))
        plo = pbt - phi * 128.0
        shi = jnp.floor(sdt * (1.0 / 128.0))
        slo = sdt - shi * 128.0
        for k in range(8):
            lanes = slice(128 * k, 128 * (k + 1))
            oh[0:C_BLK, lanes] = onehot(ic == pct[k : k + 1, :])
            mb[0:1, lanes] = phi[k : k + 1, :].astype(BF16)
            mb[1:2, lanes] = plo[k : k + 1, :].astype(BF16)
            mb[2:3, lanes] = shi[k : k + 1, :].astype(BF16)
            mb[3:4, lanes] = slo[k : k + 1, :].astype(BF16)
            mb[4:5, lanes] = jnp.ones((1, 128), BF16)
        ohb = oh[0:C_BLK, :]
        rows = pl.ds(pl.multiple_of(b * C_BLK, 16), C_BLK)
        xcm[rows, 0:LAT] = dot_nn(ohb, el[pl.ds(pl.multiple_of(b * BLK, BLK), BLK), :]).astype(BF16)
        meta = dot_nt(ohb, mb[...])
        xcm[rows, LAT : LAT + 128] = meta.astype(BF16)
        metac[rows, :] = jnp.broadcast_to(
            meta[:, 0:1] * 128.0 + meta[:, 1:2] + (meta[:, 4:5] - 1.0), (C_BLK, 128)
        )
        return 0

    lax.fori_loop(0, 8, compact, 0)
    for k in range(NCOMP // 128):
        pcrow[:, 128 * k : 128 * (k + 1)] = jnp.broadcast_to(
            row_of(metac[128 * k : 128 * (k + 1), :]), (8, 128)
        )

    for c in q_copies:
        c.wait_recv()
    for s in range(NP):
        b, c = base_of(s), cap_of(s)
        for j in range(-(-c // 128)):
            n = min(128, c - 128 * j)
            srow[0:1, b + 128 * j : b + 128 * j + n] = reqr[s, j : j + 1, 0:n]
    flag_p = jnp.max(reqr[:, 7, :], axis=0, keepdims=True)
    flagr[h] = jnp.broadcast_to(flag_p, (8, 128))
    il640 = iota((128, SUB), 1)
    for k in range(NROW // 128):
        soh[128 * k : 128 * (k + 1), :] = onehot(il640 == col_of(srow[0:1, 128 * k : 128 * (k + 1)]))

    def serve_rows(c, _):
        rows = pl.ds(pl.multiple_of(c * 2 * MCH, 16), 2 * MCH)
        serve[rows, :] = dot_nn(soh[rows, :], blk[...]).astype(BF16)
        return 0

    lax.fori_loop(0, NROW // (2 * MCH), serve_rows, 0)
    order = (1, 15) + tuple(range(2, 15))
    g_copies = []
    for s in order:
        rows = pl.ds(base_of(s), cap_of(s))
        c = remote(
            serve.at[rows], recvrows.at[rows], g_ss.at[s], g_rs.at[s], (lax.rem(p + NP - s, NP), h)
        )
        c.start()
        g_copies.append(c)
    ownr = slice(base_of(0), base_of(0) + C_OWN)
    recvrows[ownr, :] = serve[ownr, :]
    fl_copies = [
        remote(flagr.at[h], flagr.at[h], fl_ss.at[d], fl_rs.at[d], (p, hp(d))) for d in range(1, NH)
    ]
    for c in fl_copies:
        c.start()
    isub = iota((SUB, 128), 0)
    for k in range(NROW // 128):
        scoh[:, 128 * k : 128 * (k + 1)] = onehot(isub == srow[0:1, 128 * k : 128 * (k + 1)])
    forward(0)

    def arrange(c, _):
        rows = pl.ds(pl.multiple_of(c * MCH, 16), MCH)
        j0 = (c * MCH).astype(F32)
        perm = onehot(iota((MCH, NCOMP), 0) + j0 == pcrow[0:1, :])
        x = dot_nn(perm, xcm[...])
        xb[rows, :] = x[:, 0:LAT].astype(BF16)
        pick = x[:, LAT + 2 : LAT + 3] * 128.0 + x[:, LAT + 3 : LAT + 4]
        pre[rows, :] = dot_nn(onehot(iota((MCH, GRID), 1) == pick), grid[...])
        return 0

    lax.fori_loop(0, NROW // MCH, arrange, 0)
    weights_ready(0)
    lane = lax.broadcasted_iota(jnp.int32, (8, 128), 1)
    for j in range(4):
        even, odd = tbr[2 * j, 8:16, :], tbr[2 * j + 1, 8:16, :]
        vecs[:, 128 * j : 128 * (j + 1)] = jnp.where(lane < LW, even, odd)

    def full(k):
        return wfull[:, k].reshape(LAT, LAT)

    def first(c, _):
        rows = pl.ds(pl.multiple_of(c * MCH, 16), MCH)
        pre[rows, :] = dot_nt(xb[rows, :], full(0)) + dot_nt(pre[rows, :].astype(BF16), full(1)) + vecs[0:1, :]
        return 0

    lax.fori_loop(0, NROW // MCH, first, 0)
    for c in g_copies:
        c.wait_recv()

    def mlp(c, _):
        rows = pl.ds(pl.multiple_of(c * MCH, 16), MCH)
        v = pre[rows, :] + dot_nt(recvrows[rows, :], full(2))
        hid = silu(v).astype(BF16)
        msg = norm_rows(dot_nn(hid, full(3)) + vecs[1:2, :], vecs[2:3, :], vecs[3:4, :])
        msgb[rows, :] = msg.astype(BF16)
        eob[rows, :] = (xb[rows, :].astype(F32) + msg).astype(BF16)
        return 0

    lax.fori_loop(0, NROW // MCH, mlp, 0)
    m_copies = []
    for s in order:
        rows = pl.ds(base_of(s), cap_of(s))
        c = remote(msgb.at[rows], mrecv.at[rows], m_ss.at[s], m_rs.at[s], (pp(s), h))
        c.start()
        m_copies.append(c)
    mrecv[ownr, :] = msgb[ownr, :]
    forward(1)

    def scatter_block(d, _):
        b = lax.rem(h + d, NH)
        rows = pl.ds(pl.multiple_of(b * C_BLK, 16), C_BLK)
        mine = pl.ds(pl.multiple_of(h * C_BLK, 16), C_BLK)
        perm = onehot(iota((C_BLK, NROW), 1) == metac[rows, 0:1])
        eoc[rows, :] = dot_nn(perm, eob[...]).astype(BF16)

        @pl.when(d > 0)
        def _():
            remote(eoc.at[rows], recvx.at[mine], x_ss.at[d], x_rs.at[d], (p, b)).start()

        @pl.when(d == 0)
        def _():
            recvx[mine, :] = eoc[rows, :]

        return 0

    lax.fori_loop(0, NH, scatter_block, 0)

    for c in m_copies:
        c.wait_recv()
    weights_ready(1)

    def sums(c, _):
        rows = pl.ds(pl.multiple_of(c * 128, 128), 128)
        summed[rows, :] = dot_nn(scoh[rows, :], mrecv[...]).astype(BF16)
        return 0

    lax.fori_loop(0, SUB // 128, sums, 0)

    def mesh(c, _):
        rows = pl.ds(pl.multiple_of(c * 128, 128), 128)
        x = blk[rows, :]
        v = dot_nt(x, full(4)) + dot_nt(summed[rows, :], full(5)) + vecs[4:5, :]
        hid = silu(v).astype(BF16)
        upd = norm_rows(dot_nn(hid, full(6)) + vecs[5:6, :], vecs[6:7, :], vecs[7:8, :])
        mot[:, rows] = (x.astype(F32) + upd).T.astype(BF16)
        return 0

    lax.fori_loop(0, SUB // 128, mesh, 0)
    mo_copies = []
    at_mesh = pl.ds(pl.multiple_of(h * SUB, 128), SUB)
    for d in range(1, NH):
        c = remote(
            mot.at[pl.ds(pl.multiple_of(hp(d) * LW, LW), LW), :], mo_hbm.at[:, at_mesh],
            mo_ss.at[d], mo_rs.at[d], (p, hp(d)),
        )
        c.start()
        mo_copies.append(c)
    mo_own = pltpu.make_async_copy(
        mot.at[pl.ds(pl.multiple_of(h * LW, LW), LW), :], mo_hbm.at[:, at_mesh], lsem.at[3]
    )
    mo_own.start()

    subt = sub_ref[pl.ds(h8, 8), :]
    i8 = iota((8, 128), 0)
    for k in range(8):
        m2_ref[8 * k : 8 * k + 8, :] = jnp.where(i8 == subt[k : k + 1, :], 1.0, 0.0)
    rk2 = dot_nn(m2_ref[...].astype(BF16), tri)
    seen = jnp.zeros((8, 128), F32)
    for k in range(8):
        rank = rk2[8 * k : 8 * k + 8, :128] + seen
        seen = seen + rk2[8 * k : 8 * k + 8, 128:]
        px = jnp.sum(m2_ref[8 * k : 8 * k + 8, :] * (i8 * float(C_BLK) + rank), axis=0, keepdims=True)
        posx[128 * k : 128 * (k + 1), :] = jnp.broadcast_to(
            col_of(jnp.where(subt[k : k + 1, :] >= 0.0, px, -1.0)), (128, 128)
        )
    for d in range(1, NH):
        src = pl.ds(pl.multiple_of(lax.rem(h + NH - d, NH) * C_BLK, 16), C_BLK)
        remote(recvx.at[src], recvx.at[src], x_ss.at[d], x_rs.at[d], (p, hp(d))).wait_recv()

    def edge_rows(c, _):
        slots = pl.ds(pl.multiple_of(c * 128, 128), 128)
        px = posx[slots, :]
        perm = onehot(iota((128, NCOMP), 1) == px[:, 0:1])
        moved = dot_nn(perm, recvx[...])
        at = pl.ds(pl.multiple_of(h * BLK + c * 128, 128), 128)
        out = jnp.where(px[:, 0:1] >= 0.0, moved, el[at, :].astype(F32))
        eot[:, slots] = out.T.astype(BF16)
        return 0

    lax.fori_loop(0, BLK // 128, edge_rows, 0)
    eo_copies = []
    at_edge = pl.ds(pl.multiple_of(h * BLK, 128), BLK)
    for d in range(1, NH):
        c = remote(
            eot.at[pl.ds(pl.multiple_of(hp(d) * LW, LW), LW), :], eo_hbm.at[:, at_edge],
            eo_ss.at[d], eo_rs.at[d], (p, hp(d)),
        )
        c.start()
        eo_copies.append(c)
    eo_own = pltpu.make_async_copy(
        eot.at[pl.ds(pl.multiple_of(h * LW, LW), LW), :], eo_hbm.at[:, at_edge], lsem.at[4]
    )
    eo_own.start()

    for d in range(1, NH):
        src = lax.rem(h + NH - d, NH)
        remote(flagr.at[src], flagr.at[src], fl_ss.at[d], fl_rs.at[d], (p, hp(d))).wait_recv()
    flag_ref[...] = jnp.max(flagr[...], axis=0)
    for c in t_copies + w_copies + q_copies + g_copies + fl_copies + m_copies:
        c.wait_send()
    for part in range(2):
        for d in (1, 3, 2):
            from_chip(part, d)[1].wait_send()
    for d in range(1, NH):
        rows = pl.ds(pl.multiple_of(hp(d) * C_BLK, 16), C_BLK)
        remote(eoc.at[rows], eoc.at[rows], x_ss.at[d], x_rs.at[d], (p, hp(d))).wait_send()
    for d in range(1, NH):
        src_h = lax.rem(h + NH - d, NH)
        at_m = pl.ds(pl.multiple_of(src_h * SUB, 128), SUB)
        at_e = pl.ds(pl.multiple_of(src_h * BLK, 128), BLK)
        remote(mo_hbm.at[:, at_m], mo_hbm.at[:, at_m], mo_ss.at[d], mo_rs.at[d], (p, hp(d))).wait_recv()
        remote(eo_hbm.at[:, at_e], eo_hbm.at[:, at_e], eo_ss.at[d], eo_rs.at[d], (p, hp(d))).wait_recv()
    for c in mo_copies + eo_copies:
        c.wait_send()
    mo_own.wait()
    eo_own.wait()


def sparse_step(grid_latent, mesh_latent, edge_latent, senders, receivers, mesh_slot, edge_counts,
                w_edge, w_sender, w_receiver, edge_bias, w_edge_out, edge_out_bias, edge_gain, edge_shift,
                w_mesh_in, w_message_in, mesh_bias, w_mesh_out, mesh_out_bias, mesh_gain, mesh_shift):
    V = pltpu.VMEM
    vm = pl.BlockSpec(memory_space=pltpu.VMEM)
    anyspec = pl.BlockSpec(memory_space=pl.ANY)
    weights = (w_edge.T, w_sender.T, w_receiver.T, w_edge_out, w_mesh_in.T, w_message_in.T, w_mesh_out)
    vectors = tuple(v.reshape(1, LW) for v in (
        edge_bias, edge_out_bias, edge_gain, edge_shift, mesh_bias, mesh_out_bias, mesh_gain, mesh_shift))
    dma = pltpu.SemaphoreType.DMA
    scratch = [
        V((EDGE, LAT), BF16), V((GRID, LAT), BF16), V((SUB, LAT), BF16), V((NH, 7, LW, LAT), BF16),
        V((16, 128), F32), V((NH, 16, 128), F32), V((TAB, 1024), BF16),
        V((64, 128), F32), V((64, 128), F32), V((64, 128), F32), V((64, 128), F32),
        V((1024, 128), BF16), V((1024, 256), F32), V((64, 256), F32),
        V((64, 128), F32), V((64, 128), F32), V((96, 1024), BF16), V((128, 1024), BF16),
        V((96, 128), F32), V((NP, 8, 128), F32), V((NP, 8, 128), F32), V((128, 1024), BF16),
        V((64, 128), F32), V((BLK, 128), F32),
        V((NCOMP, LAT + 128), BF16), V((NCOMP, 128), F32), V((NROW, LAT), BF16), V((NROW, LAT), F32),
        V((8, NROW), F32), V((NROW, SUB), BF16), V((NROW, LAT), BF16), V((NROW, LAT), BF16),
        V((SUB, NROW), BF16), V((NROW, LAT), BF16), V((NROW, LAT), BF16), V((NROW, LAT), BF16),
        V((8, NCOMP), F32), V((NCOMP, LAT), BF16), V((NCOMP, LAT), BF16),
        V((LAT, SUB), BF16), V((LAT, BLK), BF16), V((SUB, LAT), BF16), V((8, LAT), F32), V((NH, 8, 128), F32),
        dma((5,)), dma((7,)), dma((8,)), dma((8,)), dma((8,)), dma((8,)), dma((8,)), dma((8,)),
        dma((16,)), dma((16,)), dma((16,)), dma((16,)), dma((16,)), dma((16,)),
        dma((8,)), dma((8,)), dma((8,)), dma((8,)), dma((8,)), dma((8,)), dma((8,)), dma((8,)),
    ]
    mo_t, eo_t, flag = pl.pallas_call(
        kernel,
        out_shape=(
            jax.ShapeDtypeStruct((LW, MESH), BF16),
            jax.ShapeDtypeStruct((LW, EDGE), BF16),
            jax.ShapeDtypeStruct((8, 128), F32),
        ),
        in_specs=[vm, vm, vm, pl.BlockSpec(memory_space=pltpu.SMEM), anyspec, anyspec, anyspec]
        + [anyspec] * 7 + [vm] * 8,
        out_specs=(anyspec, anyspec, vm),
        scratch_shapes=scratch,
        compiler_params=pltpu.CompilerParams(
            collective_id=0, has_side_effects=True, vmem_limit_bytes=62 * 1024 * 1024
        ),
        name="encoder",
    )(receivers.reshape(64, 128), senders.reshape(64, 128), mesh_slot.reshape(TAB, 128), edge_counts,
      edge_latent, grid_latent, mesh_latent, *weights, *vectors)
    return mo_t, eo_t, flag


def from_everyone(x, axis):
    copies = jnp.broadcast_to(x, (lax.axis_size(axis), *x.shape))
    return lax.all_to_all(copies, axis, split_axis=0, concat_axis=0, tiled=True)


def total_of(x, axis):
    return from_everyone(x, axis).sum(axis=0)


def scatter_columns(x):
    parts = x.astype(BF16).reshape(x.shape[0], NH, LW).transpose(1, 0, 2)
    got = lax.all_to_all(parts, "hidden", split_axis=0, concat_axis=0, tiled=True)
    return got.astype(F32).sum(axis=0)


def normalize(values, gain, offset):
    center = total_of(jnp.sum(values, axis=1), "hidden") / LAT
    centered = values - center[:, None]
    spread = total_of(jnp.sum(centered * centered, axis=1), "hidden") / LAT
    return centered * lax.rsqrt(spread + EPSILON)[:, None] * gain + offset


def general_step(grid_latent, mesh_latent, edge_latent, senders, receivers, mesh_slot, edge_counts,
                 w_edge, w_sender, w_receiver, edge_bias, w_edge_out, edge_out_bias, edge_gain, edge_shift,
                 w_mesh_in, w_message_in, mesh_bias, w_mesh_out, mesh_out_bias, mesh_gain, mesh_shift):
    column = lax.axis_index("hidden")
    target = jnp.take(mesh_slot, receivers)
    sender = senders - lax.axis_index("patch") * GRID
    live = (jnp.arange(EDGE, dtype=jnp.int32) < edge_counts[0]).astype(F32)
    proj = jnp.dot(mesh_latent, w_receiver, preferred_element_type=F32).astype(BF16)
    table = from_everyone(proj, "patch").reshape(NP * MESH, LW)
    edge_pre = (
        jnp.dot(edge_latent, w_edge, preferred_element_type=F32)
        + jnp.dot(jnp.take(grid_latent, sender, axis=0), w_sender, preferred_element_type=F32)
        + jnp.take(table, target, axis=0).astype(F32)
        + edge_bias
    )
    hid = silu(edge_pre).astype(BF16)
    edge_sum = scatter_columns(jnp.dot(hid, w_edge_out, preferred_element_type=F32)) + edge_out_bias
    message = normalize(edge_sum, edge_gain, edge_shift) * live[:, None]
    cols = lax.dynamic_slice_in_dim(edge_latent, column * LW, LW, 1)
    edge_out = (cols.astype(F32) + message).astype(BF16)
    sums = jax.ops.segment_sum(message, target, num_segments=NP * MESH).astype(BF16)
    got = lax.all_to_all(sums.reshape(NP, MESH, LW), "patch", split_axis=0, concat_axis=0, tiled=True)
    own = got.astype(F32).sum(axis=0).astype(BF16)
    summed = from_everyone(own, "hidden").transpose(1, 0, 2).reshape(MESH, LAT)
    mesh_pre = (
        jnp.dot(mesh_latent, w_mesh_in, preferred_element_type=F32)
        + jnp.dot(summed, w_message_in, preferred_element_type=F32)
        + mesh_bias
    )
    hid = silu(mesh_pre).astype(BF16)
    mesh_sum = scatter_columns(jnp.dot(hid, w_mesh_out, preferred_element_type=F32)) + mesh_out_bias
    update = normalize(mesh_sum, mesh_gain, mesh_shift)
    cols = lax.dynamic_slice_in_dim(mesh_latent, column * LW, LW, 1)
    return (cols.astype(F32) + update).astype(BF16).T, edge_out.T


def step(*args):
    mo_t, eo_t, flag = sparse_step(*args)

    def again(state):
        mo, eo = general_step(*args)
        return jnp.zeros_like(state[0]), mo, eo

    mo_t, eo_t = lax.cond(flag[0, 0] > 0.5, lambda: general_step(*args), lambda: (mo_t, eo_t))
    return mo_t.T, eo_t.T


def solution(mesh):
    return jax.shard_map(
        step,
        mesh=mesh,
        in_specs=(
            P("patch", None), P("patch", None), P("patch", None), P("patch"), P("patch"), P(), P("patch"),
            P(None, "hidden"), P(None, "hidden"), P(None, "hidden"), P("hidden"), P("hidden", None),
            P("hidden"), P("hidden"), P("hidden"), P(None, "hidden"), P(None, "hidden"), P("hidden"),
            P("hidden", None), P("hidden"), P("hidden"), P("hidden"),
        ),
        out_specs=(P("patch", "hidden"), P("patch", "hidden")),
        check_vma=False,
    )
```

```python
import jax
import jax.numpy as jnp
from jax import lax
from jax.experimental import pallas as pl
from jax.experimental.pallas import tpu as pltpu
from jax.sharding import PartitionSpec as P

EPSILON = 1e-05
F32 = jnp.float32
BF16 = jnp.bfloat16
NP = 16
NH = 8
LAT = 512
GRID = 3072
EDGE = 8192
MESH = 5120
SUB = MESH // NH
BLK = EDGE // NH
LW = LAT // NH
TAB = NP * MESH // 128
C_OWN, C_NEAR, C_FAR = 384, 224, 64
C_BLK = 176
NROW = C_OWN + 2 * C_NEAR + 13 * C_FAR
NCOMP = NH * C_BLK
MCH = 208
SCH = 352
EARLY = 8
FCH = 704
PCH = 416
UCH = 512
HALF = NCOMP // 2
DEV = pl.DeviceIdType.MESH
GROUPS = ((5, 6, 7, 8, 9, 10, 11), (2, 3, 4, 12, 13, 14), (1, 15))


def base_of(s):
    if s == 0:
        return NROW - C_OWN
    if s in (1, 15):
        return 13 * C_FAR + (C_NEAR if s == 15 else 0)
    if s < 5:
        return C_FAR * (7 + s - 2)
    if s > 11:
        return C_FAR * (10 + s - 12)
    return C_FAR * (s - 5)


def cap_of(s):
    return C_OWN if s == 0 else (C_NEAR if s in (1, 15) else C_FAR)


def iota(shape, dim):
    return lax.broadcasted_iota(jnp.int32, shape, dim).astype(F32)


def dot_nn(a, b):
    return lax.dot_general(a, b, (((1,), (0,)), ((), ())), preferred_element_type=F32)


def dot_nt(a, b):
    return lax.dot_general(a, b, (((1,), (1,)), ((), ())), preferred_element_type=F32)


def onehot(mask):
    return jnp.where(mask, 1.0, 0.0).astype(BF16)


def col_of(row):
    eye = iota((128, 128), 0) == iota((128, 128), 1)
    return jnp.sum(jnp.where(eye, row, 0.0), axis=1, keepdims=True)


def row_of(col):
    eye = iota((128, 128), 0) == iota((128, 128), 1)
    return jnp.sum(jnp.where(eye, col, 0.0), axis=0, keepdims=True)


def norm_rows(values, gain, offset):
    center = jnp.sum(values, axis=1, keepdims=True) * (1.0 / LAT)
    centered = values - center
    spread = jnp.sum(centered * centered, axis=1, keepdims=True) * (1.0 / LAT)
    return centered * lax.rsqrt(spread + EPSILON) * gain + offset


def silu(v):
    return v / (1.0 + jnp.exp(-v))


def kernel(
    recv_i, send_i, slot, cnt, el_hbm, grid_hbm, mesh_hbm,
    w0, w1, w2, w3, w4, w5, w6,
    b0, b1, b2, b3, b4, b5, b6, b7,
    mo_hbm, eo_hbm, flag_ref,
    el, grid, blk, wfull, tb, tbr, oh, tabt, t_ref, s_ref, sub_ref, r_ref, sd_ref, m_ref, rk_ref, o_ref,
    posb, posc, aq, bq, req_acc, req, reqr, m2_ref, posx,
    xc, sc, prec, metac, pre, srow, soh, serve, recvrows, scoh, msgb, mrecv, pcrow, eoc, xs, xr,
    mot, eot, summed, mrow, vecs, flagr,
    lsem, wlsem, t_ss, t_rs, w_ss, w_rs, f_ss, f_rs, q_ss, q_rs, g_ss, g_rs, m_ss, m_rs,
    x_ss, x_rs, mo_ss, mo_rs, fl_ss, fl_rs,
):
    p = lax.axis_index("patch")
    h = lax.axis_index("hidden")
    hf = h.astype(F32)
    pf = p.astype(F32)

    def hp(d):
        return lax.rem(h + d, NH)

    def pp(s):
        return lax.rem(p + s, NP)

    def remote(src, dst, ss, rs, dev):
        return pltpu.make_async_remote_copy(
            src_ref=src, dst_ref=dst, send_sem=ss, recv_sem=rs, device_id=dev, device_id_type=DEV
        )
    loads = [
        pltpu.make_async_copy(
            mesh_hbm.at[pl.ds(pl.multiple_of(h * SUB, SUB), SUB), :], blk, lsem.at[2]
        ),
        pltpu.make_async_copy(el_hbm, el, lsem.at[0]),
        pltpu.make_async_copy(grid_hbm, grid, lsem.at[1]),
    ]
    wsrc = (w0, w1, w2, w3, w4, w5, w6)
    wl = [pltpu.make_async_copy(wsrc[k], wfull.at[h, k], wlsem.at[k]) for k in range(7)]
    for c in wl:
        c.start()
    for c in loads:
        c.start()
    barrier = pltpu.get_barrier_semaphore()
    for d in range(1, NH):
        pl.semaphore_signal(barrier, inc=1, device_id=(p, hp(d)), device_id_type=DEV)
    for s in range(1, NP):
        pl.semaphore_signal(barrier, inc=1, device_id=(pp(s), h), device_id_type=DEV)
    i128 = iota((128, 128), 0)
    i256 = iota((256, 128), 0)
    vt = slot[...].astype(F32).T
    va = jnp.floor(vt * (1.0 / 256.0))
    vb = (vt - va * 256.0).astype(BF16)
    va = (va - 256.0).astype(BF16)
    tabt[512:768, :] = jnp.zeros((256, 256), BF16)
    for k in range(3):
        n = min(256, TAB - 256 * k)
        tabt[256 * k : 256 * k + 128, 0:n] = va[:, 256 * k : 256 * k + n]
        tabt[256 * k + 128 : 256 * k + 256, 0:n] = vb[:, 256 * k : 256 * k + n]

    def lookup(b, _):
        rr = recv_i[pl.ds(pl.multiple_of(b * 8, 8), 8), :]
        rhi = (lax.shift_right_logical(rr, 7) & 255).astype(F32)
        rtop = lax.shift_right_logical(rr, 15).astype(F32)
        rlo = (rr & 127).astype(F32)
        for k in range(8):
            oh[:, 128 * k : 128 * (k + 1)] = onehot(i256 == rhi[k : k + 1, :])
        pair = dot_nn(tabt[...], oh[...])
        for k in range(8):
            lanes = slice(128 * k, 128 * (k + 1))
            t0 = rtop[k : k + 1, :] == 0.0
            t1 = rtop[k : k + 1, :] == 1.0
            pa = jnp.where(t0, pair[0:128, lanes], jnp.where(t1, pair[256:384, lanes], pair[512:640, lanes]))
            pb = jnp.where(t0, pair[128:256, lanes], jnp.where(t1, pair[384:512, lanes], pair[640:768, lanes]))
            t_ref[pl.ds(b * 8 + k, 1), :] = jnp.sum(
                jnp.where(i128 == rlo[k : k + 1, :], (pa + 256.0) * 256.0 + pb, 0.0), axis=0, keepdims=True
            )
        return 0

    lax.fori_loop(0, 8, lookup, 0)
    for k, b in enumerate((b0, b1, b2, b3, b4, b5, b6, b7)):
        tb[k : k + 1, 0:LW] = b[...]
        tb[k : k + 1, LW:128] = b[...]
    for c in wl:
        c.wait()
    pl.semaphore_wait(barrier, NH - 1 + NP - 1)
    t_copies = [
        remote(tb, tbr.at[h], t_ss.at[d], t_rs.at[d], (p, hp(d))) for d in range(1, NH)
    ]
    for c in t_copies:
        c.start()
    tbr[h] = tb[...]
    parity = lax.rem(h, 2)
    partner = h + 1 - 2 * parity
    ahead = 2 - 4 * parity
    w_copies = []

    def along(part, i):
        lo, n = ((0, 4), (4, 3))[part]
        src_h, dst_h = ((h, h + 2), (h, h + NH - 2), (h - ahead + NH, h + ahead + NH))[i]
        ref = wfull.at[lax.rem(src_h, NH), pl.ds(lo, n)]
        return remote(ref, ref, w_ss.at[part * 4 + i], w_rs.at[part * 4 + i], (p, lax.rem(dst_h, NH)))

    def arrived(part, i):
        lo, n = ((0, 4), (4, 3))[part]
        ref = wfull.at[lax.rem(h + (NH - 2, 2, 4)[i], NH), pl.ds(lo, n)]
        remote(ref, ref, w_ss.at[part * 4 + i], w_rs.at[part * 4 + i], (p, partner)).wait_recv()

    def across(part, i, base):
        lo, n = ((0, 4), (4, 3))[part]
        ref = wfull.at[lax.rem(base + (0, NH - 2, 2, 4)[i], NH), pl.ds(lo, n)]
        return remote(ref, ref, f_ss.at[part * 4 + i], f_rs.at[part * 4 + i], (p, partner))

    def begin(c):
        c.start()
        w_copies.append(c)

    def stage0(part):
        begin(along(part, 0))
        begin(along(part, 1))
        begin(across(part, 0, h))

    def stage1(part):
        arrived(part, 0)
        arrived(part, 1)
        begin(along(part, 2))
        begin(across(part, 1, h))
        begin(across(part, 2, h))

    def stage2(part):
        arrived(part, 2)
        begin(across(part, 3, h))

    def weights_ready(part):
        for i in range(4):
            across(part, i, partner).wait_recv()

    stage0(0)

    tri = jnp.where(iota((128, 256), 1) < 128.0,
                    jnp.where(iota((128, 256), 0) < iota((128, 256), 1), 1.0, 0.0), 1.0).astype(BF16)
    i16 = iota((16, 128), 0)
    base16 = jnp.zeros((16, 128), F32)
    for s in range(NP):
        base16 = jnp.where(i16 == float(s), float(base_of(s)), base16)
    cap16 = jnp.where(i16 == 0.0, float(C_OWN), jnp.where((i16 == 1.0) | (i16 == 15.0), float(C_NEAR), float(C_FAR)))
    i48 = iota((48, 128), 0)
    tf = t_ref[...]
    q = jnp.floor((tf + 0.5) * (1.0 / MESH))
    rem = tf - q * MESH
    sub = jnp.floor((rem + 0.5) * (1.0 / SUB))
    r1 = rem - sub * SUB + 1.0
    shift = q - pf
    shift = jnp.where(shift < 0.0, shift + NP, shift)
    eidx = lax.broadcasted_iota(jnp.int32, (64, 128), 0) * 128 + lax.broadcasted_iota(jnp.int32, (64, 128), 1)
    live = eidx < cnt[0]
    own = live & (sub == hf)
    s_ref[...] = jnp.where(own, shift, -1.0)
    r_ref[...] = r1
    sd_ref[...] = (send_i[...] - p * GRID).astype(F32)
    spread = jnp.where(live, sub, lax.rem(eidx, NH).astype(F32))
    sub_ref[...] = spread
    o_ref[...] = dot_nn(onehot(spread == hf), tri)

    def mark(b, _):
        st = s_ref[pl.ds(pl.multiple_of(b * 8, 8), 8), :]
        for k in range(8):
            m_ref[pl.ds(pl.multiple_of(b * 128 + 16 * k, 16), 16), :] = onehot(i16 == st[k : k + 1, :])
        return 0

    lax.fori_loop(0, 8, mark, 0)
    rk_ref[...] = dot_nn(m_ref[...], tri)
    def place(b, carry):
        counts, most = carry
        b8 = pl.ds(pl.multiple_of(b * 8, 8), 8)
        st = s_ref[b8, :]
        rt = r_ref[b8, :]
        ot = o_ref[b8, :]
        sb = sub_ref[b8, :]
        rowcount = jnp.zeros((1, 128), F32)
        pbs, pcs = [], []
        vhi = jnp.floor(rt * (1.0 / 256.0))
        vlo = rt - vhi * 256.0
        for k in range(8):
            i0 = pl.ds(pl.multiple_of(b * 128 + 16 * k, 16), 16)
            rk = rk_ref[i0, :]
            mk = m_ref[i0, :].astype(F32)
            rank = rk[:, :128] + counts
            counts = counts + rk[:, 128:]
            isown = st[k : k + 1, :] >= 0.0
            pb = jnp.sum(mk * (base16 + rank), axis=0, keepdims=True)
            rk1 = jnp.sum(mk * rank, axis=0, keepdims=True)
            pbs.append(jnp.where(isown, pb, -1.0))
            pcs.append(jnp.where(sb[k : k + 1, :] == hf, ot[k : k + 1, :128] + rowcount, -1.0))
            rowcount = rowcount + ot[k : k + 1, 128:]
            qhi0 = jnp.floor(rk1 * (1.0 / 128.0))
            qlo = rk1 - qhi0 * 128.0
            qhi = jnp.where(isown & (qhi0 < 3.0), st[k : k + 1, :] * 3.0 + qhi0, -1.0)
            hit = i48 == qhi
            lanes = pl.ds(pl.multiple_of(b * 1024 + 128 * k, 128), 128)
            aq[0:48, lanes] = jnp.where(hit, vhi[k : k + 1, :], 0.0).astype(BF16)
            aq[48:96, lanes] = jnp.where(hit, vlo[k : k + 1, :], 0.0).astype(BF16)
            bq[:, lanes] = onehot(i128 == qlo)
        for k in range(8):
            posb[pl.ds(b * 8 + k, 1), :] = pbs[k]
            posc[pl.ds(b * 8 + k, 1), :] = pcs[k]
        return counts, jnp.maximum(most, rowcount)

    counts, most = lax.fori_loop(0, 8, place, (jnp.zeros((16, 128), F32), jnp.zeros((1, 128), F32)))
    req_acc[...] = dot_nt(aq[...], bq[...])
    over = jnp.max(jnp.where(counts > cap16, 1.0, 0.0), axis=0, keepdims=True)
    over = jnp.maximum(over, jnp.where(most > float(C_BLK), 1.0, 0.0))
    for s in range(NP):
        req[s, 0:3, :] = req_acc[3 * s : 3 * s + 3, :] * 256.0 + req_acc[48 + 3 * s : 48 + 3 * s + 3, :] - 1.0
        req[s, 3:7, :] = jnp.full((4, 128), -1.0, F32)
        req[s, 7:8, :] = over
    q_copies = [
        remote(req.at[s], reqr.at[s], q_ss.at[s], q_rs.at[s], (pp(s), h)) for s in range(1, NP)
    ]
    for c in q_copies:
        c.start()
    reqr[0] = req[0]
    for c in loads:
        c.wait()
    ic = iota((C_BLK, 128), 0)

    def compact(b, _):
        b8 = pl.ds(pl.multiple_of(b * 8, 8), 8)
        pct = posc[b8, :]
        pbt = posb[b8, :] + 1.0
        sdt = sd_ref[b8, :]
        at_b = jnp.zeros((C_BLK, 128), F32)
        at_s = jnp.zeros((C_BLK, 128), F32)
        for k in range(8):
            hit = ic == pct[k : k + 1, :]
            oh[0:C_BLK, 128 * k : 128 * (k + 1)] = onehot(hit)
            at_b = at_b + jnp.where(hit, pbt[k : k + 1, :], 0.0)
            at_s = at_s + jnp.where(hit, sdt[k : k + 1, :], 0.0)
        rows = pl.ds(pl.multiple_of(b * C_BLK, 16), C_BLK)
        xc[rows, :] = dot_nn(oh[0:C_BLK, :], el[pl.ds(pl.multiple_of(b * BLK, BLK), BLK), :]).astype(BF16)
        lanes = lax.broadcasted_iota(jnp.int32, (C_BLK, 128), 1)
        metac[rows, :] = jnp.where(
            lanes < 64,
            jnp.sum(at_b, axis=1, keepdims=True) - 1.0,
            jnp.sum(at_s, axis=1, keepdims=True),
        )
        return 0

    lax.fori_loop(0, EARLY, compact, 0)
    for k in range(NCOMP // 128):
        pcrow[:, 128 * k : 128 * (k + 1)] = jnp.broadcast_to(
            row_of(metac[128 * k : 128 * (k + 1), 0:1]), (8, 128)
        )
    for c in q_copies:
        c.wait_recv()
    stage1(0)
    for s in range(NP):
        b, c = base_of(s), cap_of(s)
        for j in range(-(-c // 128)):
            n = min(128, c - 128 * j)
            srow[0:1, b + 128 * j : b + 128 * j + n] = reqr[s, j : j + 1, 0:n]
    flag_p = jnp.max(reqr[:, 7, :], axis=0, keepdims=True)
    flagr[h] = jnp.broadcast_to(flag_p, (8, 128))
    il640 = iota((128, SUB), 1)
    for k in range(NROW // 128):
        soh[128 * k : 128 * (k + 1), :] = onehot(il640 == col_of(srow[0:1, 128 * k : 128 * (k + 1)]))
    def serve_rows(c, _):
        rows = pl.ds(pl.multiple_of(c * 2 * MCH, 16), 2 * MCH)
        serve[rows, :] = dot_nn(soh[rows, :], blk[...]).astype(BF16)
        return 0

    lax.fori_loop(0, NROW // (2 * MCH), serve_rows, 0)
    order = sum(GROUPS, ())
    g_copies = []
    for s in order:
        rows = pl.ds(base_of(s), cap_of(s))
        c = remote(
            serve.at[rows], recvrows.at[rows], g_ss.at[s], g_rs.at[s], (lax.rem(p + NP - s, NP), h)
        )
        c.start()
        g_copies.append(c)
    ownr = slice(base_of(0), base_of(0) + C_OWN)
    recvrows[ownr, :] = serve[ownr, :]
    fl_copies = [
        remote(flagr.at[h], flagr.at[h], fl_ss.at[d], fl_rs.at[d], (p, hp(d))) for d in range(1, NH)
    ]
    for c in fl_copies:
        c.start()
    isub = iota((SUB, 128), 0)
    for k in range(NROW // 128):
        scoh[:, 128 * k : 128 * (k + 1)] = onehot(isub == srow[0:1, 128 * k : 128 * (k + 1)])
    def gather_senders(c, _):
        rows = pl.ds(pl.multiple_of(c * SCH, 16), SCH)
        pick = metac[rows, 64:65]
        sc[rows, :] = dot_nn(onehot(iota((SCH, GRID), 1) == pick), grid[...]).astype(BF16)
        return 0

    lax.fori_loop(0, NCOMP // SCH, gather_senders, 0)
    stage2(0)
    stage0(1)
    weights_ready(0)
    for c in t_copies:
        c.wait_recv()
    lane = lax.broadcasted_iota(jnp.int32, (8, 128), 1)
    for j in range(4):
        even, odd = tbr[2 * j], tbr[2 * j + 1]
        vecs[:, 128 * j : 128 * (j + 1)] = jnp.where(lane < LW, even, odd)

    def full(k):
        return wfull[:, k].reshape(LAT, LAT)

    def first(c, _):
        rows = pl.ds(pl.multiple_of(c * FCH, 16), FCH)
        prec[rows, :] = (dot_nt(xc[rows, :], full(0)) + dot_nt(sc[rows, :], full(1)) + vecs[0:1, :]).astype(BF16)
        return 0

    lax.fori_loop(0, NCOMP // FCH, first, 0)

    def arrange(c, _):
        rows = pl.ds(pl.multiple_of(c * PCH, 16), PCH)
        j0 = (c * PCH).astype(F32)
        pre[rows, :] = dot_nn(onehot(iota((PCH, NCOMP), 0) + j0 == pcrow[0:1, :]), prec[...])
        return 0

    lax.fori_loop(0, NROW // PCH, arrange, 0)

    def mlp(start, n):
        rows = slice(start, start + n)
        v = pre[rows, :] + dot_nt(recvrows[rows, :], full(2))
        hid = silu(v).astype(BF16)
        msg = norm_rows(dot_nn(hid, full(3)) + vecs[1:2, :], vecs[2:3, :], vecs[3:4, :])
        msgb[rows, :] = msg.astype(BF16)
    stage1(1)
    mlp(base_of(0), C_OWN // 2)
    mlp(base_of(0) + C_OWN // 2, C_OWN // 2)
    mrecv[ownr, :] = msgb[ownr, :]
    m_copies = []
    g_wait = dict(zip(order, g_copies))
    for gi, group in enumerate(GROUPS):
        for s in group:
            g_wait[s].wait_recv()
        start = base_of(group[0])
        n = sum(cap_of(s) for s in group)
        mlp(start, n // 2)
        mlp(start + n // 2, n - n // 2)
        for s in group:
            rows = pl.ds(base_of(s), cap_of(s))
            c = remote(msgb.at[rows], mrecv.at[rows], m_ss.at[s], m_rs.at[s], (pp(s), h))
            c.start()
            m_copies.append(c)
    stage2(1)


    def scatter_block(c, _):
        rows = pl.ds(pl.multiple_of(c * SCH, 16), SCH)
        perm = onehot(iota((SCH, NROW), 1) == metac[rows, 0:1])
        eoc[rows, :] = (xc[rows, :].astype(F32) + dot_nn(perm, msgb[...])).astype(BF16)
        return 0

    lax.fori_loop(0, NCOMP // SCH, scatter_block, 0)
    low = lax.broadcasted_iota(jnp.int32, (HALF, 128), 1) < LW
    for j in range(4):
        cols = slice(128 * j, 128 * (j + 1))
        top = eoc[0:HALF, cols].astype(F32)
        bottom = eoc[HALF:NCOMP, cols].astype(F32)
        xs[2 * j] = jnp.where(low, top, pltpu.roll(bottom, LW, 1)).astype(BF16)
        xs[2 * j + 1] = jnp.where(low, pltpu.roll(top, LW, 1), bottom).astype(BF16)
    x_copies = []
    for half in range(2):
        part = pl.ds(half * HALF // 2, HALF // 2)
        for d in range(1, NH):
            i = half * 8 + d
            c = remote(xs.at[hp(d), part], xr.at[h, part], x_ss.at[i], x_rs.at[i], (p, hp(d)))
            c.start()
            x_copies.append(c)
    xr[h] = xs[h]

    i8 = iota((8, 128), 0)

    def mark2(b, _):
        st = sub_ref[pl.ds(pl.multiple_of(b * 8, 8), 8), :]
        for k in range(8):
            m2_ref[pl.ds(pl.multiple_of(b * 64 + 8 * k, 8), 8), :] = jnp.where(i8 == st[k : k + 1, :], 1.0, 0.0)
        return 0

    lax.fori_loop(0, 8, mark2, 0)
    rk_ref[0:512, :] = dot_nn(m2_ref[...].astype(BF16), tri)

    def place2(b, _):
        seen = jnp.zeros((8, 128), F32)
        for k in range(8):
            i0 = pl.ds(pl.multiple_of(b * 64 + 8 * k, 8), 8)
            rk = rk_ref[i0, :]
            rank = rk[:, :128] + seen
            seen = seen + rk[:, 128:]
            posx[pl.ds(b * 8 + k, 1), :] = jnp.sum(
                m2_ref[i0, :] * (i8 * float(C_BLK) + rank), axis=0, keepdims=True
            )
        return 0

    lax.fori_loop(0, 8, place2, 0)
    lane_low = lax.broadcasted_iota(jnp.int32, (UCH, 128), 1) < LW

    def rows_arrived(half):
        for d in range(1, NH):
            src = xr.at[lax.rem(h + NH - d, NH), pl.ds(half * HALF // 2, HALF // 2)]
            remote(src, src, x_ss.at[half * 8 + d], x_rs.at[half * 8 + d], (p, hp(d))).wait_recv()

    def edge_rows(t, _):
        b = t // (BLK // UCH)
        c = t - b * (BLK // UCH)
        x2 = xr[:, pl.ds(pl.multiple_of(b * C_BLK, 16), C_BLK), :].reshape(NCOMP, 128)
        x2 = jnp.concatenate([x2[0:HALF], x2[HALF:NCOMP]], axis=1)
        perms = []
        tops = []
        for block in (b, b + 4):
            for k in range(UCH // 128):
                col = col_of(posx[pl.ds(block * 8 + c * (UCH // 128) + k, 1), :])
                top = col >= float(HALF)
                tops.append(jnp.broadcast_to(jnp.where(top, 1.0, 0.0), (128, 128)))
                perms.append(onehot(iota((128, HALF), 1) == jnp.where(top, col - float(HALF), col)))
        got = dot_nn(jnp.concatenate(perms, axis=0), x2)
        got = jnp.where(jnp.concatenate(tops, axis=0) > 0.5, got[:, 128:256], got[:, 0:128])
        both = jnp.where(lane_low, got[0:UCH], got[UCH : 2 * UCH]).T.astype(BF16)
        eot[:, pl.ds(pl.multiple_of(b * BLK + c * UCH, 128), UCH)] = both[0:LW]
        eot[:, pl.ds(pl.multiple_of((b + 4) * BLK + c * UCH, 128), UCH)] = both[LW:128]
        return 0

    per_half = 2 * (BLK // UCH)

    for c in m_copies:
        c.wait_recv()
    weights_ready(1)
    for c in range(2):
        rows = slice(c * SUB // 2, (c + 1) * SUB // 2)
        summed[rows, :] = dot_nn(scoh[rows, :], mrecv[...]).astype(BF16)

    def mesh(c, _):
        rows = pl.ds(pl.multiple_of(c * (SUB // 2), 16), SUB // 2)
        x = blk[rows, :]
        v = dot_nt(x, full(4)) + dot_nt(summed[rows, :], full(5)) + vecs[4:5, :]
        hid = silu(v).astype(BF16)
        upd = norm_rows(dot_nn(hid, full(6)) + vecs[5:6, :], vecs[6:7, :], vecs[7:8, :])
        mrow[rows, :] = x.astype(F32) + upd
        return 0

    lax.fori_loop(0, 2, mesh, 0)

    def turn(c, _):
        rows = pl.ds(pl.multiple_of(c * 128, 128), 128)
        mot[:, rows] = mrow[rows, :].T.astype(BF16)
        return 0

    lax.fori_loop(0, SUB // 128, turn, 0)
    mo_copies = []
    at_mesh = pl.ds(pl.multiple_of(h * SUB, 128), SUB)
    for d in range(1, NH):
        c = remote(
            mot.at[pl.ds(pl.multiple_of(hp(d) * LW, LW), LW), :], mo_hbm.at[:, at_mesh],
            mo_ss.at[d], mo_rs.at[d], (p, hp(d)),
        )
        c.start()
        mo_copies.append(c)
    mo_own = pltpu.make_async_copy(
        mot.at[pl.ds(pl.multiple_of(h * LW, LW), LW), :], mo_hbm.at[:, at_mesh], lsem.at[3]
    )
    mo_own.start()
    rows_arrived(0)
    lax.fori_loop(0, per_half, edge_rows, 0)
    rows_arrived(1)
    lax.fori_loop(per_half, 2 * per_half, edge_rows, 0)
    eo_own = pltpu.make_async_copy(eot, eo_hbm, lsem.at[4])
    eo_own.start()
    for d in range(1, NH):
        src = lax.rem(h + NH - d, NH)
        remote(flagr.at[src], flagr.at[src], fl_ss.at[d], fl_rs.at[d], (p, hp(d))).wait_recv()
    flag_ref[...] = jnp.max(flagr[...], axis=0)
    for c in t_copies + w_copies + q_copies + g_copies + fl_copies + m_copies + x_copies + mo_copies:
        c.wait_send()
    for d in range(1, NH):
        src_h = lax.rem(h + NH - d, NH)
        at_m = pl.ds(pl.multiple_of(src_h * SUB, 128), SUB)
        remote(mo_hbm.at[:, at_m], mo_hbm.at[:, at_m], mo_ss.at[d], mo_rs.at[d], (p, hp(d))).wait_recv()
    mo_own.wait()
    eo_own.wait()


def sparse_step(grid_latent, mesh_latent, edge_latent, senders, receivers, mesh_slot, edge_counts,
                w_edge, w_sender, w_receiver, edge_bias, w_edge_out, edge_out_bias, edge_gain, edge_shift,
                w_mesh_in, w_message_in, mesh_bias, w_mesh_out, mesh_out_bias, mesh_gain, mesh_shift):
    V = pltpu.VMEM
    vm = pl.BlockSpec(memory_space=pltpu.VMEM)
    anyspec = pl.BlockSpec(memory_space=pl.ANY)
    weights = (w_edge.T, w_sender.T, w_receiver.T, w_edge_out, w_mesh_in.T, w_message_in.T, w_mesh_out)
    vectors = tuple(v.reshape(1, LW) for v in (
        edge_bias, edge_out_bias, edge_gain, edge_shift, mesh_bias, mesh_out_bias, mesh_gain, mesh_shift))
    dma = pltpu.SemaphoreType.DMA
    scratch = [
        V((EDGE, LAT), BF16), V((GRID, LAT), BF16), V((SUB, LAT), BF16), V((NH, 7, LW, LAT), BF16),
        V((8, 128), F32), V((NH, 8, 128), F32), V((256, 1024), BF16), V((768, 256), BF16), V((64, 128), F32),
        V((64, 128), F32), V((64, 128), F32), V((64, 128), F32), V((64, 128), F32),
        V((1024, 128), BF16), V((1024, 256), F32), V((64, 256), F32),
        V((64, 128), F32), V((64, 128), F32), V((96, EDGE), BF16), V((128, EDGE), BF16),
        V((96, 128), F32), V((NP, 8, 128), F32), V((NP, 8, 128), F32),
        V((512, 128), F32), V((64, 128), F32),
        V((NCOMP, LAT), BF16), V((NCOMP, LAT), BF16), V((NCOMP, LAT), BF16), V((NCOMP, 128), F32), V((NROW, LAT), F32),
        V((8, NROW), F32), V((NROW, SUB), BF16), V((NROW, LAT), BF16), V((NROW, LAT), BF16),
        V((SUB, NROW), BF16), V((NROW, LAT), BF16), V((NROW, LAT), BF16),
        V((8, NCOMP), F32), V((NCOMP, LAT), BF16), V((NH, HALF, 128), BF16), V((NH, HALF, 128), BF16),
        V((LAT, SUB), BF16), V((LW, EDGE), BF16), V((SUB, LAT), BF16), V((SUB, LAT), F32), V((8, LAT), F32), V((NH, 8, 128), F32),
        dma((5,)), dma((7,)), dma((8,)), dma((8,)), dma((8,)), dma((8,)), dma((8,)), dma((8,)),
        dma((16,)), dma((16,)), dma((16,)), dma((16,)), dma((16,)), dma((16,)),
        dma((16,)), dma((16,)), dma((8,)), dma((8,)), dma((8,)), dma((8,)),
    ]
    mo_t, eo_t, flag = pl.pallas_call(
        kernel,
        out_shape=(
            jax.ShapeDtypeStruct((LW, MESH), BF16),
            jax.ShapeDtypeStruct((LW, EDGE), BF16),
            jax.ShapeDtypeStruct((8, 128), F32),
        ),
        in_specs=[vm, vm, vm, pl.BlockSpec(memory_space=pltpu.SMEM), anyspec, anyspec, anyspec]
        + [anyspec] * 7 + [vm] * 8,
        out_specs=(anyspec, anyspec, vm),
        scratch_shapes=scratch,
        compiler_params=pltpu.CompilerParams(
            collective_id=0, has_side_effects=True, vmem_limit_bytes=62 * 1024 * 1024
        ),
        name="encoder",
    )(receivers.reshape(64, 128), senders.reshape(64, 128), mesh_slot.reshape(TAB, 128), edge_counts,
      edge_latent, grid_latent, mesh_latent, *weights, *vectors)
    return mo_t, eo_t, flag


def from_everyone(x, axis):
    copies = jnp.broadcast_to(x, (lax.axis_size(axis), *x.shape))
    return lax.all_to_all(copies, axis, split_axis=0, concat_axis=0, tiled=True)


def total_of(x, axis):
    return from_everyone(x, axis).sum(axis=0)


def scatter_columns(x):
    parts = x.astype(BF16).reshape(x.shape[0], NH, LW).transpose(1, 0, 2)
    got = lax.all_to_all(parts, "hidden", split_axis=0, concat_axis=0, tiled=True)
    return got.astype(F32).sum(axis=0)


def normalize(values, gain, offset):
    center = total_of(jnp.sum(values, axis=1), "hidden") / LAT
    centered = values - center[:, None]
    spread = total_of(jnp.sum(centered * centered, axis=1), "hidden") / LAT
    return centered * lax.rsqrt(spread + EPSILON)[:, None] * gain + offset


def general_step(grid_latent, mesh_latent, edge_latent, senders, receivers, mesh_slot, edge_counts,
                 w_edge, w_sender, w_receiver, edge_bias, w_edge_out, edge_out_bias, edge_gain, edge_shift,
                 w_mesh_in, w_message_in, mesh_bias, w_mesh_out, mesh_out_bias, mesh_gain, mesh_shift):
    column = lax.axis_index("hidden")
    target = jnp.take(mesh_slot, receivers)
    sender = senders - lax.axis_index("patch") * GRID
    live = (jnp.arange(EDGE, dtype=jnp.int32) < edge_counts[0]).astype(F32)
    proj = jnp.dot(mesh_latent, w_receiver, preferred_element_type=F32).astype(BF16)
    table = from_everyone(proj, "patch").reshape(NP * MESH, LW)
    edge_pre = (
        jnp.dot(edge_latent, w_edge, preferred_element_type=F32)
        + jnp.dot(jnp.take(grid_latent, sender, axis=0), w_sender, preferred_element_type=F32)
        + jnp.take(table, target, axis=0).astype(F32)
        + edge_bias
    )
    hid = silu(edge_pre).astype(BF16)
    edge_sum = scatter_columns(jnp.dot(hid, w_edge_out, preferred_element_type=F32)) + edge_out_bias
    message = normalize(edge_sum, edge_gain, edge_shift) * live[:, None]
    cols = lax.dynamic_slice_in_dim(edge_latent, column * LW, LW, 1)
    edge_out = (cols.astype(F32) + message).astype(BF16)
    sums = jax.ops.segment_sum(message, target, num_segments=NP * MESH).astype(BF16)
    got = lax.all_to_all(sums.reshape(NP, MESH, LW), "patch", split_axis=0, concat_axis=0, tiled=True)
    own = got.astype(F32).sum(axis=0).astype(BF16)
    summed = from_everyone(own, "hidden").transpose(1, 0, 2).reshape(MESH, LAT)
    mesh_pre = (
        jnp.dot(mesh_latent, w_mesh_in, preferred_element_type=F32)
        + jnp.dot(summed, w_message_in, preferred_element_type=F32)
        + mesh_bias
    )
    hid = silu(mesh_pre).astype(BF16)
    mesh_sum = scatter_columns(jnp.dot(hid, w_mesh_out, preferred_element_type=F32)) + mesh_out_bias
    update = normalize(mesh_sum, mesh_gain, mesh_shift)
    cols = lax.dynamic_slice_in_dim(mesh_latent, column * LW, LW, 1)
    return (cols.astype(F32) + update).astype(BF16).T, edge_out.T


def step(*args):
    mo_t, eo_t, flag = sparse_step(*args)

    def again(state):
        mo, eo = general_step(*args)
        return jnp.zeros_like(state[0]), mo, eo

    mo_t, eo_t = lax.cond(flag[0, 0] > 0.5, lambda: general_step(*args), lambda: (mo_t, eo_t))
    return mo_t.T, eo_t.T


def solution(mesh):
    return jax.shard_map(
        step,
        mesh=mesh,
        in_specs=(
            P("patch", None), P("patch", None), P("patch", None), P("patch"), P("patch"), P(), P("patch"),
            P(None, "hidden"), P(None, "hidden"), P(None, "hidden"), P("hidden"), P("hidden", None),
            P("hidden"), P("hidden"), P("hidden"), P(None, "hidden"), P(None, "hidden"), P("hidden"),
            P("hidden", None), P("hidden"), P("hidden"), P("hidden"),
        ),
        out_specs=(P("patch", "hidden"), P("patch", "hidden")),
        check_vma=False,
    )
```

```python
import jax
import jax.numpy as jnp
from jax import lax
from jax.experimental import pallas as pl
from jax.experimental.pallas import tpu as pltpu
from jax.sharding import PartitionSpec as P

EPSILON = 1e-05
F32 = jnp.float32
BF16 = jnp.bfloat16
NP = 16
NH = 8
LAT = 512
GRID = 3072
EDGE = 8192
MESH = 5120
SUB = MESH // NH
BLK = EDGE // NH
LW = LAT // NH
TAB = NP * MESH // 128
C_OWN, C_NEAR, C_FAR = 384, 224, 64
C_BLK = 176
NROW = C_OWN + 2 * C_NEAR + 13 * C_FAR
NCOMP = NH * C_BLK
MCH = 208
SCH = 352
EARLY = 8
FCH = 704
PCH = 416
UCH = 512
HALF = NCOMP // 2
DEV = pl.DeviceIdType.MESH
PARTS = ((0, 2), (2, 2), (4, 3))
GROUPS = ((5, 6, 7, 8, 9, 10, 11), (2, 3, 4, 12, 13, 14), (1, 15))


def base_of(s):
    if s == 0:
        return NROW - C_OWN
    if s in (1, 15):
        return 13 * C_FAR + (C_NEAR if s == 15 else 0)
    if s < 5:
        return C_FAR * (7 + s - 2)
    if s > 11:
        return C_FAR * (10 + s - 12)
    return C_FAR * (s - 5)


def cap_of(s):
    return C_OWN if s == 0 else (C_NEAR if s in (1, 15) else C_FAR)


def iota(shape, dim):
    return lax.broadcasted_iota(jnp.int32, shape, dim).astype(F32)


def dot_nn(a, b):
    return lax.dot_general(a, b, (((1,), (0,)), ((), ())), preferred_element_type=F32)


def dot_nt(a, b):
    return lax.dot_general(a, b, (((1,), (1,)), ((), ())), preferred_element_type=F32)


def onehot(mask):
    return jnp.where(mask, 1.0, 0.0).astype(BF16)


def col_of(row):
    eye = iota((128, 128), 0) == iota((128, 128), 1)
    return jnp.sum(jnp.where(eye, row, 0.0), axis=1, keepdims=True)


def row_of(col):
    eye = iota((128, 128), 0) == iota((128, 128), 1)
    return jnp.sum(jnp.where(eye, col, 0.0), axis=0, keepdims=True)


def norm_rows(values, gain, offset):
    center = jnp.sum(values, axis=1, keepdims=True) * (1.0 / LAT)
    centered = values - center
    spread = jnp.sum(centered * centered, axis=1, keepdims=True) * (1.0 / LAT)
    return centered * lax.rsqrt(spread + EPSILON) * gain + offset


def silu(v):
    return v / (1.0 + jnp.exp(-v))


def kernel(
    recv_i, send_i, slot, cnt, el_hbm, grid_hbm, mesh_hbm,
    w0, w1, w2, w3, w4, w5, w6,
    b0, b1, b2, b3, b4, b5, b6, b7,
    mo_hbm, eo_hbm, flag_hbm,
    el, grid, blk, wfull, tb, tbr, oh, tabt, t_ref, s_ref, sub_ref, r_ref, sd_ref, m_ref, rk_ref, o_ref,
    posb, posc, aq, bq, req_acc, req, reqr, m2_ref, posx,
    xc, sc, prec, metac, pre, srow, soh, serve, recvrows, scoh, msgb, mrecv, pcrow, eoc, xs, xr,
    mot, eot, mpre, mrow, vecs, flagr, flag_v,
    lsem, snd, rcv,
):
    p = lax.axis_index("patch")
    h = lax.axis_index("hidden")
    hf = h.astype(F32)
    pf = p.astype(F32)

    def hp(d):
        return lax.rem(h + d, NH)

    def pp(s):
        return lax.rem(p + s, NP)

    def remote(src, dst, ss, rs, dev):
        return pltpu.make_async_remote_copy(
            src_ref=src, dst_ref=dst, send_sem=ss, recv_sem=rs, device_id=dev, device_id_type=DEV
        )
    def got(ref, i):
        remote(ref, ref, snd.at[0], rcv.at[i], (p, h + 1 - 2 * lax.rem(h, 2))).wait_recv()

    def sent(ref, i):
        remote(ref, ref, snd.at[i], rcv.at[0], (p, h + 1 - 2 * lax.rem(h, 2))).wait_send()

    loads = [
        pltpu.make_async_copy(
            mesh_hbm.at[pl.ds(pl.multiple_of(h * SUB, SUB), SUB), :], blk, lsem.at[2]
        ),
        pltpu.make_async_copy(el_hbm, el, lsem.at[0]),
        pltpu.make_async_copy(grid_hbm, grid, lsem.at[1]),
    ]
    wsrc = (w0, w1, w2, w3, w4, w5, w6)
    wl = [pltpu.make_async_copy(wsrc[k], wfull.at[h, k], lsem.at[3]) for k in range(7)]
    for c in wl:
        c.start()
    for c in loads:
        c.start()
    barrier = pltpu.get_barrier_semaphore()
    for d in range(1, NH):
        pl.semaphore_signal(barrier, inc=1, device_id=(p, hp(d)), device_id_type=DEV)
    for s in range(1, NP):
        pl.semaphore_signal(barrier, inc=1, device_id=(pp(s), h), device_id_type=DEV)
    i128 = iota((128, 128), 0)
    i256 = iota((256, 128), 0)
    vt = slot[...].astype(F32).T
    va = jnp.floor(vt * (1.0 / 256.0))
    vb = (vt - va * 256.0).astype(BF16)
    va = (va - 256.0).astype(BF16)
    tabt[512:768, :] = jnp.zeros((256, 256), BF16)
    for k in range(3):
        n = min(256, TAB - 256 * k)
        tabt[256 * k : 256 * k + 128, 0:n] = va[:, 256 * k : 256 * k + n]
        tabt[256 * k + 128 : 256 * k + 256, 0:n] = vb[:, 256 * k : 256 * k + n]

    parity = lax.rem(h, 2)
    partner = h + 1 - 2 * parity

    def lookup(b, _):
        rr = recv_i[pl.ds(pl.multiple_of(b * 8, 8), 8), :]
        rhi = (lax.shift_right_logical(rr, 7) & 255).astype(F32)
        rtop = lax.shift_right_logical(rr, 15).astype(F32)
        rlo = (rr & 127).astype(F32)
        for k in range(8):
            oh[:, 128 * k : 128 * (k + 1)] = onehot(i256 == rhi[k : k + 1, :])
        pair = dot_nn(tabt[...], oh[...])
        for k in range(8):
            lanes = slice(128 * k, 128 * (k + 1))
            t0 = rtop[k : k + 1, :] == 0.0
            t1 = rtop[k : k + 1, :] == 1.0
            pa = jnp.where(t0, pair[0:128, lanes], jnp.where(t1, pair[256:384, lanes], pair[512:640, lanes]))
            pb = jnp.where(t0, pair[128:256, lanes], jnp.where(t1, pair[384:512, lanes], pair[640:768, lanes]))
            t_ref[pl.ds(b * 8 + k, 1), :] = jnp.sum(
                jnp.where(i128 == rlo[k : k + 1, :], (pa + 256.0) * 256.0 + pb, 0.0), axis=0, keepdims=True
            )
        return 0

    lax.fori_loop(parity * 4, parity * 4 + 4, lookup, 0)
    for k, b in enumerate((b0, b1, b2, b3, b4, b5, b6, b7)):
        tb[k : k + 1, 0:LW] = b[...]
        tb[k : k + 1, LW:128] = b[...]
    pltpu.make_async_copy(wfull.at[h], wfull.at[h], lsem.at[3]).wait()
    pl.semaphore_wait(barrier, NH - 1 + NP - 1)
    own_half = t_ref.at[pl.ds(pl.multiple_of(parity * 32, 32), 32), :]
    other_half = t_ref.at[pl.ds(pl.multiple_of(32 - parity * 32, 32), 32), :]
    swap = remote(own_half, own_half, snd.at[0], rcv.at[0], (p, partner))
    swap.start()
    t_copies = [
        remote(tb, tbr.at[h], snd.at[1], rcv.at[1], (p, hp(d))) for d in range(1, NH)
    ]
    for c in t_copies:
        c.start()
    tbr[h] = tb[...]
    ahead = 2 - 4 * parity
    w_copies = []

    def along(part, i):
        lo, n = PARTS[part]
        src_h, dst_h = ((h, h + 2), (h, h + NH - 2), (h - ahead + NH, h + ahead + NH))[i]
        ref = wfull.at[lax.rem(src_h, NH), pl.ds(lo, n)]
        return remote(ref, ref, snd.at[2], rcv.at[12 + 2 * part + i // 2], (p, lax.rem(dst_h, NH)))

    def arrived(part, i):
        lo, n = PARTS[part]
        got(wfull.at[0 : 2 - i, pl.ds(lo, n)], 12 + 2 * part + i)

    def across(part, i, base):
        lo, n = PARTS[part]
        ref = wfull.at[lax.rem(base + (0, NH - 2, 2, 4)[i], NH), pl.ds(lo, n)]
        return remote(ref, ref, snd.at[3], rcv.at[18 + part], (p, partner))

    def begin(c):
        c.start()
        w_copies.append(c)

    def stage0(part):
        begin(along(part, 0))
        begin(along(part, 1))
        begin(across(part, 0, h))

    def stage1(part):
        arrived(part, 0)
        begin(along(part, 2))
        begin(across(part, 1, h))
        begin(across(part, 2, h))

    def stage2(part):
        arrived(part, 1)
        begin(across(part, 3, h))

    def weights_ready(part):
        lo, n = PARTS[part]
        got(wfull.at[0:4, pl.ds(lo, n)], 18 + part)

    stage0(0)
    stage0(1)

    tri = jnp.where(iota((128, 256), 1) < 128.0,
                    jnp.where(iota((128, 256), 0) < iota((128, 256), 1), 1.0, 0.0), 1.0).astype(BF16)
    i16 = iota((16, 128), 0)
    base16 = jnp.zeros((16, 128), F32)
    for s in range(NP):
        base16 = jnp.where(i16 == float(s), float(base_of(s)), base16)
    cap16 = jnp.where(i16 == 0.0, float(C_OWN), jnp.where((i16 == 1.0) | (i16 == 15.0), float(C_NEAR), float(C_FAR)))
    i48 = iota((48, 128), 0)
    got(other_half, 0)
    tf = t_ref[...]
    q = jnp.floor((tf + 0.5) * (1.0 / MESH))
    rem = tf - q * MESH
    sub = jnp.floor((rem + 0.5) * (1.0 / SUB))
    r1 = rem - sub * SUB + 1.0
    shift = q - pf
    shift = jnp.where(shift < 0.0, shift + NP, shift)
    eidx = lax.broadcasted_iota(jnp.int32, (64, 128), 0) * 128 + lax.broadcasted_iota(jnp.int32, (64, 128), 1)
    live = eidx < cnt[0]
    own = live & (sub == hf)
    s_ref[...] = jnp.where(own, shift, -1.0)
    r_ref[...] = r1
    sd_ref[...] = (send_i[...] - p * GRID).astype(F32)
    spread = jnp.where(live, sub, lax.rem(eidx, NH).astype(F32))
    sub_ref[...] = spread
    o_ref[...] = dot_nn(onehot(spread == hf), tri)

    def mark(b, _):
        st = s_ref[pl.ds(pl.multiple_of(b * 8, 8), 8), :]
        for k in range(8):
            m_ref[pl.ds(pl.multiple_of(b * 128 + 16 * k, 16), 16), :] = onehot(i16 == st[k : k + 1, :])
        return 0

    lax.fori_loop(0, 8, mark, 0)
    rk_ref[...] = dot_nn(m_ref[...], tri)
    def place(b, carry):
        counts, most = carry
        b8 = pl.ds(pl.multiple_of(b * 8, 8), 8)
        st = s_ref[b8, :]
        rt = r_ref[b8, :]
        ot = o_ref[b8, :]
        sb = sub_ref[b8, :]
        rowcount = jnp.zeros((1, 128), F32)
        pbs, pcs = [], []
        vhi = jnp.floor(rt * (1.0 / 256.0))
        vlo = rt - vhi * 256.0
        for k in range(8):
            i0 = pl.ds(pl.multiple_of(b * 128 + 16 * k, 16), 16)
            rk = rk_ref[i0, :]
            mk = m_ref[i0, :].astype(F32)
            rank = rk[:, :128] + counts
            counts = counts + rk[:, 128:]
            isown = st[k : k + 1, :] >= 0.0
            pb = jnp.sum(mk * (base16 + rank), axis=0, keepdims=True)
            rk1 = jnp.sum(mk * rank, axis=0, keepdims=True)
            pbs.append(jnp.where(isown, pb, -1.0))
            pcs.append(jnp.where(sb[k : k + 1, :] == hf, ot[k : k + 1, :128] + rowcount, -1.0))
            rowcount = rowcount + ot[k : k + 1, 128:]
            qhi0 = jnp.floor(rk1 * (1.0 / 128.0))
            qlo = rk1 - qhi0 * 128.0
            qhi = jnp.where(isown & (qhi0 < 3.0), st[k : k + 1, :] * 3.0 + qhi0, -1.0)
            hit = i48 == qhi
            lanes = pl.ds(pl.multiple_of(b * 1024 + 128 * k, 128), 128)
            aq[0:48, lanes] = jnp.where(hit, vhi[k : k + 1, :], 0.0).astype(BF16)
            aq[48:96, lanes] = jnp.where(hit, vlo[k : k + 1, :], 0.0).astype(BF16)
            bq[:, lanes] = onehot(i128 == qlo)
        for k in range(8):
            posb[pl.ds(b * 8 + k, 1), :] = pbs[k]
            posc[pl.ds(b * 8 + k, 1), :] = pcs[k]
        return counts, jnp.maximum(most, rowcount)

    counts, most = lax.fori_loop(0, 8, place, (jnp.zeros((16, 128), F32), jnp.zeros((1, 128), F32)))
    req_acc[...] = dot_nt(aq[...], bq[...])
    over = jnp.max(jnp.where(counts > cap16, 1.0, 0.0), axis=0, keepdims=True)
    over = jnp.maximum(over, jnp.where(most > float(C_BLK), 1.0, 0.0))
    for s in range(NP):
        req[s, 0:3, :] = req_acc[3 * s : 3 * s + 3, :] * 256.0 + req_acc[48 + 3 * s : 48 + 3 * s + 3, :] - 1.0
        req[s, 3:7, :] = jnp.full((4, 128), -1.0, F32)
        req[s, 7:8, :] = over
    q_copies = [
        remote(req.at[s], reqr.at[s], snd.at[4], rcv.at[2], (pp(s), h)) for s in range(1, NP)
    ]
    for c in q_copies:
        c.start()
    reqr[0] = req[0]
    for c in loads:
        c.wait()
    ic = iota((C_BLK, 128), 0)

    def compact(b, _):
        b8 = pl.ds(pl.multiple_of(b * 8, 8), 8)
        pct = posc[b8, :]
        pbt = posb[b8, :] + 1.0
        sdt = sd_ref[b8, :]
        at_b = jnp.zeros((C_BLK, 128), F32)
        at_s = jnp.zeros((C_BLK, 128), F32)
        for k in range(8):
            hit = ic == pct[k : k + 1, :]
            oh[0:C_BLK, 128 * k : 128 * (k + 1)] = onehot(hit)
            at_b = at_b + jnp.where(hit, pbt[k : k + 1, :], 0.0)
            at_s = at_s + jnp.where(hit, sdt[k : k + 1, :], 0.0)
        rows = pl.ds(pl.multiple_of(b * C_BLK, 16), C_BLK)
        xc[rows, :] = dot_nn(oh[0:C_BLK, :], el[pl.ds(pl.multiple_of(b * BLK, BLK), BLK), :]).astype(BF16)
        lanes = lax.broadcasted_iota(jnp.int32, (C_BLK, 128), 1)
        metac[rows, :] = jnp.where(
            lanes < 64,
            jnp.sum(at_b, axis=1, keepdims=True) - 1.0,
            jnp.sum(at_s, axis=1, keepdims=True),
        )
        return 0

    lax.fori_loop(0, 8, compact, 0)
    stage1(0)
    for k in range(NCOMP // 128):
        pcrow[:, 128 * k : 128 * (k + 1)] = jnp.broadcast_to(
            row_of(metac[128 * k : 128 * (k + 1), 0:1]), (8, 128)
        )

    i8 = iota((8, 128), 0)

    def mark2(b, _):
        st = sub_ref[pl.ds(pl.multiple_of(b * 8, 8), 8), :]
        for k in range(8):
            m2_ref[pl.ds(pl.multiple_of(b * 64 + 8 * k, 8), 8), :] = jnp.where(i8 == st[k : k + 1, :], 1.0, 0.0)
        return 0

    lax.fori_loop(0, 8, mark2, 0)
    rk_ref[0:512, :] = dot_nn(m2_ref[...].astype(BF16), tri)

    def place2(b, _):
        seen = jnp.zeros((8, 128), F32)
        for k in range(8):
            i0 = pl.ds(pl.multiple_of(b * 64 + 8 * k, 8), 8)
            rk = rk_ref[i0, :]
            rank = rk[:, :128] + seen
            seen = seen + rk[:, 128:]
            posx[pl.ds(b * 8 + k, 1), :] = jnp.sum(
                m2_ref[i0, :] * (i8 * float(C_BLK) + rank), axis=0, keepdims=True
            )
        return 0

    lax.fori_loop(0, 8, place2, 0)
    got(reqr.at[1:NP], 2)
    for s in range(NP):
        b, c = base_of(s), cap_of(s)
        for j in range(-(-c // 128)):
            n = min(128, c - 128 * j)
            srow[0:1, b + 128 * j : b + 128 * j + n] = reqr[s, j : j + 1, 0:n]
    flag_p = jnp.max(reqr[:, 7, :], axis=0, keepdims=True)
    flagr[h] = jnp.broadcast_to(flag_p, (8, 128))
    il640 = iota((128, SUB), 1)
    order = sum(GROUPS, ())
    ownr = slice(base_of(0), base_of(0) + C_OWN)
    g_copies = []

    def pick_rows(lo, hi):
        for k in range(lo, hi):
            soh[128 * k : 128 * (k + 1), :] = onehot(il640 == col_of(srow[0:1, 128 * k : 128 * (k + 1)]))

    ready = 0
    for gi, group in enumerate(GROUPS):
        upto = -(-(base_of(group[-1]) + cap_of(group[-1])) // 128)
        pick_rows(ready, upto)
        ready = upto
        b = base_of(group[0])
        n = sum(cap_of(s) for s in group)
        serve[b : b + n, :] = dot_nn(soh[b : b + n, :], blk[...]).astype(BF16)
        for s in group:
            rows = pl.ds(base_of(s), cap_of(s))
            c = remote(
                serve.at[rows], recvrows.at[rows], snd.at[5], rcv.at[4 + gi], (lax.rem(p + NP - s, NP), h)
            )
            c.start()
            g_copies.append(c)
    fl_copies = [
        remote(flagr.at[h], flagr.at[h], snd.at[9], rcv.at[3], (p, hp(d))) for d in range(1, NH)
    ]
    for c in fl_copies:
        c.start()
    stage1(1)
    stage0(2)
    pick_rows(ready, NROW // 128)
    recvrows[ownr, :] = dot_nn(soh[ownr, :], blk[...]).astype(BF16)
    isub = iota((SUB, 128), 0)
    for k in range(NROW // 128):
        scoh[:, 128 * k : 128 * (k + 1)] = onehot(isub == srow[0:1, 128 * k : 128 * (k + 1)])
    def gather_senders(c, _):
        rows = pl.ds(pl.multiple_of(c * SCH, 16), SCH)
        pick = metac[rows, 64:65]
        sc[rows, :] = dot_nn(onehot(iota((SCH, GRID), 1) == pick), grid[...]).astype(BF16)
        return 0

    lax.fori_loop(0, 2, gather_senders, 0)
    stage2(0)
    lax.fori_loop(2, NCOMP // SCH, gather_senders, 0)
    stage2(1)
    weights_ready(0)
    got(tbr.at[1:NH], 1)
    lane = lax.broadcasted_iota(jnp.int32, (8, 128), 1)
    for j in range(4):
        even, odd = tbr[2 * j], tbr[2 * j + 1]
        vecs[:, 128 * j : 128 * (j + 1)] = jnp.where(lane < LW, even, odd)

    def full(k):
        return wfull[:, k].reshape(LAT, LAT)

    def first(c, _):
        rows = pl.ds(pl.multiple_of(c * FCH, 16), FCH)
        prec[rows, :] = (dot_nt(xc[rows, :], full(0)) + dot_nt(sc[rows, :], full(1)) + vecs[0:1, :]).astype(BF16)
        return 0

    lax.fori_loop(0, NCOMP // FCH, first, 0)

    def arrange(c, _):
        rows = pl.ds(pl.multiple_of(c * PCH, 16), PCH)
        j0 = (c * PCH).astype(F32)
        pre[rows, :] = dot_nn(onehot(iota((PCH, NCOMP), 0) + j0 == pcrow[0:1, :]), prec[...])
        return 0

    lax.fori_loop(0, NROW // PCH, arrange, 0)

    def mlp(start, n):
        rows = slice(start, start + n)
        v = pre[rows, :] + dot_nt(recvrows[rows, :], full(2))
        hid = silu(v).astype(BF16)
        msg = norm_rows(dot_nn(hid, full(3)) + vecs[1:2, :], vecs[2:3, :], vecs[3:4, :])
        msgb[rows, :] = msg.astype(BF16)
    weights_ready(1)
    stage1(2)
    mlp(base_of(0), C_OWN // 2)
    mlp(base_of(0) + C_OWN // 2, C_OWN // 2)
    mrecv[ownr, :] = msgb[ownr, :]
    m_copies = []
    for gi, group in enumerate(GROUPS):
        start = base_of(group[0])
        n = sum(cap_of(s) for s in group)
        got(recvrows.at[start : start + n], 4 + gi)
        start = base_of(group[0])
        n = sum(cap_of(s) for s in group)
        mlp(start, n // 2)
        mlp(start + n // 2, n - n // 2)
        for s in group:
            rows = pl.ds(base_of(s), cap_of(s))
            c = remote(msgb.at[rows], mrecv.at[rows], snd.at[6], rcv.at[7 + gi // 2], (pp(s), h))
            c.start()
            m_copies.append(c)


    def scatter_block(c, _):
        rows = pl.ds(pl.multiple_of(c * SCH, 16), SCH)
        perm = onehot(iota((SCH, NROW), 1) == metac[rows, 0:1])
        eoc[rows, :] = (xc[rows, :].astype(F32) + dot_nn(perm, msgb[...])).astype(BF16)
        return 0

    x_copies = []
    low = lax.broadcasted_iota(jnp.int32, (HALF // 2, 128), 1) < LW
    for half in range(2):
        scatter_block(jnp.int32(half), 0)
        scatter_block(jnp.int32(half + 2), 0)
        part = pl.ds(half * HALF // 2, HALF // 2)
        for j in range(4):
            cols = slice(128 * j, 128 * (j + 1))
            top = eoc[part, cols].astype(F32)
            bottom = eoc[pl.ds(HALF + half * HALF // 2, HALF // 2), cols].astype(F32)
            xs[2 * j, part, :] = jnp.where(low, top, pltpu.roll(bottom, LW, 1)).astype(BF16)
            xs[2 * j + 1, part, :] = jnp.where(low, pltpu.roll(top, LW, 1), bottom).astype(BF16)
        for d in range(1, NH):
            c = remote(xs.at[hp(d), part], xr.at[h, part], snd.at[7], rcv.at[9 + half], (p, hp(d)))
            c.start()
            x_copies.append(c)
    xr[h] = xs[h]

    lane_low = lax.broadcasted_iota(jnp.int32, (UCH, 128), 1) < LW

    def rows_arrived(half):
        got(xr.at[1:NH, pl.ds(half * HALF // 2, HALF // 2)], 9 + half)

    def edge_rows(t, _):
        b = t // (BLK // UCH)
        c = t - b * (BLK // UCH)
        x2 = xr[:, pl.ds(pl.multiple_of(b * C_BLK, 16), C_BLK), :].reshape(NCOMP, 128)
        x2 = jnp.concatenate([x2[0:HALF], x2[HALF:NCOMP]], axis=1)
        perms = []
        tops = []
        for block in (b, b + 4):
            for k in range(UCH // 128):
                col = col_of(posx[pl.ds(block * 8 + c * (UCH // 128) + k, 1), :])
                top = col >= float(HALF)
                tops.append(jnp.broadcast_to(jnp.where(top, 1.0, 0.0), (128, 128)))
                perms.append(onehot(iota((128, HALF), 1) == jnp.where(top, col - float(HALF), col)))
        got = dot_nn(jnp.concatenate(perms, axis=0), x2)
        got = jnp.where(jnp.concatenate(tops, axis=0) > 0.5, got[:, 128:256], got[:, 0:128])
        both = jnp.where(lane_low, got[0:UCH], got[UCH : 2 * UCH]).T.astype(BF16)
        eot[:, pl.ds(pl.multiple_of(b * BLK + c * UCH, 128), UCH)] = both[0:LW]
        eot[:, pl.ds(pl.multiple_of((b + 4) * BLK + c * UCH, 128), UCH)] = both[LW:128]
        return 0

    per_half = 2 * (BLK // UCH)
    stage2(2)
    got(mrecv.at[0 : base_of(1)], 7)
    first_k = 768
    for c in range(2):
        rows = slice(c * SUB // 2, (c + 1) * SUB // 2)
        mrow[rows, :] = dot_nn(scoh[rows, ownr], mrecv[ownr, :]) + dot_nn(scoh[rows, 0:first_k], mrecv[0:first_k, :])
    weights_ready(2)

    def mesh_first(c, _):
        rows = pl.ds(pl.multiple_of(c * (SUB // 2), 16), SUB // 2)
        mpre[rows, :] = dot_nt(blk[rows, :], full(4)) + vecs[4:5, :]
        return 0

    lax.fori_loop(0, 2, mesh_first, 0)
    got(mrecv.at[base_of(1) : base_of(0)], 8)
    mo_copies = []
    mo_own = []
    for i, (start, n) in enumerate(((0, 256), (256, 384))):
        rows = slice(start, start + n)
        rest = slice(first_k, base_of(0))
        total = (mrow[rows, :] + dot_nn(scoh[rows, rest], mrecv[rest, :])).astype(BF16)
        v = mpre[rows, :] + dot_nt(total, full(5))
        hid = silu(v).astype(BF16)
        upd = norm_rows(dot_nn(hid, full(6)) + vecs[5:6, :], vecs[6:7, :], vecs[7:8, :])
        mrow[rows, :] = blk[rows, :].astype(F32) + upd
        for k in range(start // 128, (start + n) // 128):
            lanes = slice(128 * k, 128 * (k + 1))
            mot[:, lanes] = mrow[lanes, :].T.astype(BF16)
        at = pl.ds(pl.multiple_of(h * SUB + start, 128), n)
        for d in range(1, NH):
            c = remote(
                mot.at[pl.ds(pl.multiple_of(hp(d) * LW, LW), LW), pl.ds(start, n)], mo_hbm.at[:, at],
                snd.at[8], rcv.at[11], (p, hp(d)),
            )
            c.start()
            mo_copies.append(c)
        c = pltpu.make_async_copy(
            mot.at[pl.ds(pl.multiple_of(h * LW, LW), LW), pl.ds(start, n)], mo_hbm.at[:, at], lsem.at[4]
        )
        c.start()
        mo_own.append(c)

    got(flagr.at[1:NH], 3)
    flag_v[...] = jnp.max(flagr[...], axis=0)
    flag_copy = pltpu.make_async_copy(flag_v, flag_hbm, lsem.at[6])
    flag_copy.start()
    rows_arrived(0)
    lax.fori_loop(0, per_half, edge_rows, 0)
    rows_arrived(1)
    lax.fori_loop(per_half, 2 * per_half, edge_rows, 0)
    eo_own = pltpu.make_async_copy(eot, eo_hbm, lsem.at[5])
    eo_own.start()
    sent(own_half, 0)
    sent(tbr.at[1:NH], 1)
    sent(wfull.at[0:3], 2)
    sent(wfull.at[0:4], 3)
    sent(req.at[1:NP], 4)
    sent(serve.at[0 : base_of(0)], 5)
    sent(msgb.at[0 : base_of(0)], 6)
    sent(xs.at[1:NH], 7)
    sent(mot.at[LW:LAT], 8)
    sent(flagr.at[1:NH], 9)
    got(mo_hbm.at[:, SUB:MESH], 11)
    pltpu.make_async_copy(mot.at[0:LW], mot.at[0:LW], lsem.at[4]).wait()
    eo_own.wait()
    flag_copy.wait()


def sparse_step(grid_latent, mesh_latent, edge_latent, senders, receivers, mesh_slot, edge_counts,
                w_edge, w_sender, w_receiver, edge_bias, w_edge_out, edge_out_bias, edge_gain, edge_shift,
                w_mesh_in, w_message_in, mesh_bias, w_mesh_out, mesh_out_bias, mesh_gain, mesh_shift):
    V = pltpu.VMEM
    vm = pl.BlockSpec(memory_space=pltpu.VMEM)
    anyspec = pl.BlockSpec(memory_space=pl.ANY)
    weights = (w_edge.T, w_sender.T, w_receiver.T, w_edge_out, w_mesh_in.T, w_message_in.T, w_mesh_out)
    vectors = tuple(v.reshape(1, LW) for v in (
        edge_bias, edge_out_bias, edge_gain, edge_shift, mesh_bias, mesh_out_bias, mesh_gain, mesh_shift))
    dma = pltpu.SemaphoreType.DMA
    scratch = [
        V((EDGE, LAT), BF16), V((GRID, LAT), BF16), V((SUB, LAT), BF16), V((NH, 7, LW, LAT), BF16),
        V((8, 128), F32), V((NH, 8, 128), F32), V((256, 1024), BF16), V((768, 256), BF16), V((64, 128), F32),
        V((64, 128), F32), V((64, 128), F32), V((64, 128), F32), V((64, 128), F32),
        V((1024, 128), BF16), V((1024, 256), F32), V((64, 256), F32),
        V((64, 128), F32), V((64, 128), F32), V((96, EDGE), BF16), V((128, EDGE), BF16),
        V((96, 128), F32), V((NP, 8, 128), F32), V((NP, 8, 128), F32),
        V((512, 128), F32), V((64, 128), F32),
        V((NCOMP, LAT), BF16), V((NCOMP, LAT), BF16), V((NCOMP, LAT), BF16), V((NCOMP, 128), F32), V((NROW, LAT), F32),
        V((8, NROW), F32), V((NROW, SUB), BF16), V((NROW, LAT), BF16), V((NROW, LAT), BF16),
        V((SUB, NROW), BF16), V((NROW, LAT), BF16), V((NROW, LAT), BF16),
        V((8, NCOMP), F32), V((NCOMP, LAT), BF16), V((NH, HALF, 128), BF16), V((NH, HALF, 128), BF16),
        V((LAT, SUB), BF16), V((LW, EDGE), BF16), V((SUB, LAT), F32), V((SUB, LAT), F32), V((8, LAT), F32), V((NH, 8, 128), F32), V((8, 128), F32),
        dma((7,)), dma((10,)), dma((21,)),
    ]
    mo_t, eo_t, flag = pl.pallas_call(
        kernel,
        out_shape=(
            jax.ShapeDtypeStruct((LW, MESH), BF16),
            jax.ShapeDtypeStruct((LW, EDGE), BF16),
            jax.ShapeDtypeStruct((8, 128), F32),
        ),
        in_specs=[vm, vm, vm, pl.BlockSpec(memory_space=pltpu.SMEM), anyspec, anyspec, anyspec]
        + [anyspec] * 7 + [vm] * 8,
        out_specs=(anyspec, anyspec, anyspec),
        scratch_shapes=scratch,
        compiler_params=pltpu.CompilerParams(
            collective_id=0, has_side_effects=True, vmem_limit_bytes=62 * 1024 * 1024
        ),
        name="encoder",
    )(receivers.reshape(64, 128), senders.reshape(64, 128), mesh_slot.reshape(TAB, 128), edge_counts,
      edge_latent, grid_latent, mesh_latent, *weights, *vectors)
    return mo_t, eo_t, flag


def from_everyone(x, axis):
    copies = jnp.broadcast_to(x, (lax.axis_size(axis), *x.shape))
    return lax.all_to_all(copies, axis, split_axis=0, concat_axis=0, tiled=True)


def total_of(x, axis):
    return from_everyone(x, axis).sum(axis=0)


def scatter_columns(x):
    parts = x.astype(BF16).reshape(x.shape[0], NH, LW).transpose(1, 0, 2)
    got = lax.all_to_all(parts, "hidden", split_axis=0, concat_axis=0, tiled=True)
    return got.astype(F32).sum(axis=0)


def normalize(values, gain, offset):
    center = total_of(jnp.sum(values, axis=1), "hidden") / LAT
    centered = values - center[:, None]
    spread = total_of(jnp.sum(centered * centered, axis=1), "hidden") / LAT
    return centered * lax.rsqrt(spread + EPSILON)[:, None] * gain + offset


def general_step(grid_latent, mesh_latent, edge_latent, senders, receivers, mesh_slot, edge_counts,
                 w_edge, w_sender, w_receiver, edge_bias, w_edge_out, edge_out_bias, edge_gain, edge_shift,
                 w_mesh_in, w_message_in, mesh_bias, w_mesh_out, mesh_out_bias, mesh_gain, mesh_shift):
    column = lax.axis_index("hidden")
    target = jnp.take(mesh_slot, receivers)
    sender = senders - lax.axis_index("patch") * GRID
    live = (jnp.arange(EDGE, dtype=jnp.int32) < edge_counts[0]).astype(F32)
    proj = jnp.dot(mesh_latent, w_receiver, preferred_element_type=F32).astype(BF16)
    table = from_everyone(proj, "patch").reshape(NP * MESH, LW)
    edge_pre = (
        jnp.dot(edge_latent, w_edge, preferred_element_type=F32)
        + jnp.dot(jnp.take(grid_latent, sender, axis=0), w_sender, preferred_element_type=F32)
        + jnp.take(table, target, axis=0).astype(F32)
        + edge_bias
    )
    hid = silu(edge_pre).astype(BF16)
    edge_sum = scatter_columns(jnp.dot(hid, w_edge_out, preferred_element_type=F32)) + edge_out_bias
    message = normalize(edge_sum, edge_gain, edge_shift) * live[:, None]
    cols = lax.dynamic_slice_in_dim(edge_latent, column * LW, LW, 1)
    edge_out = (cols.astype(F32) + message).astype(BF16)
    sums = jax.ops.segment_sum(message, target, num_segments=NP * MESH).astype(BF16)
    got = lax.all_to_all(sums.reshape(NP, MESH, LW), "patch", split_axis=0, concat_axis=0, tiled=True)
    own = got.astype(F32).sum(axis=0).astype(BF16)
    summed = from_everyone(own, "hidden").transpose(1, 0, 2).reshape(MESH, LAT)
    mesh_pre = (
        jnp.dot(mesh_latent, w_mesh_in, preferred_element_type=F32)
        + jnp.dot(summed, w_message_in, preferred_element_type=F32)
        + mesh_bias
    )
    hid = silu(mesh_pre).astype(BF16)
    mesh_sum = scatter_columns(jnp.dot(hid, w_mesh_out, preferred_element_type=F32)) + mesh_out_bias
    update = normalize(mesh_sum, mesh_gain, mesh_shift)
    cols = lax.dynamic_slice_in_dim(mesh_latent, column * LW, LW, 1)
    return (cols.astype(F32) + update).astype(BF16).T, edge_out.T


def step(*args):
    mo_t, eo_t, flag = sparse_step(*args)

    def again(state):
        mo, eo = general_step(*args)
        return jnp.zeros_like(state[0]), mo, eo

    mo_t, eo_t = lax.cond(flag[0, 0] > 0.5, lambda: general_step(*args), lambda: (mo_t, eo_t))
    return mo_t.T, eo_t.T


def solution(mesh):
    return jax.shard_map(
        step,
        mesh=mesh,
        in_specs=(
            P("patch", None), P("patch", None), P("patch", None), P("patch"), P("patch"), P(), P("patch"),
            P(None, "hidden"), P(None, "hidden"), P(None, "hidden"), P("hidden"), P("hidden", None),
            P("hidden"), P("hidden"), P("hidden"), P(None, "hidden"), P(None, "hidden"), P("hidden"),
            P("hidden", None), P("hidden"), P("hidden"), P("hidden"),
        ),
        out_specs=(P("patch", "hidden"), P("patch", "hidden")),
        check_vma=False,
    )
```

```python
import jax
import jax.numpy as jnp
from jax import lax
from jax.experimental import pallas as pl
from jax.experimental.pallas import tpu as pltpu
from jax.sharding import PartitionSpec as P

EPSILON = 1e-05
F32 = jnp.float32
BF16 = jnp.bfloat16
NP = 16
NH = 8
LAT = 512
GRID = 3072
EDGE = 8192
MESH = 5120
SUB = MESH // NH
BLK = EDGE // NH
LW = LAT // NH
TAB = NP * MESH // 128
C_OWN, C_NEAR, C_FAR = 384, 224, 64
C_BLK = 176
NROW = C_OWN + 2 * C_NEAR + 13 * C_FAR
NCOMP = NH * C_BLK
MCH = 208
SCH = 352
EARLY = 8
FCH = 704
PCH = 416
UCH = 512
HALF = NCOMP // 2
DEV = pl.DeviceIdType.MESH
PARTS = ((0, 2), (2, 2), (4, 3))
GROUPS = ((5, 6, 7, 8, 9, 10, 11), (2, 3, 4, 12, 13, 14), (1,), (15,))
G_SEM = (4, 5, 6, 21)


def base_of(s):
    if s == 0:
        return NROW - C_OWN
    if s in (1, 15):
        return 13 * C_FAR + (C_NEAR if s == 15 else 0)
    if s < 5:
        return C_FAR * (7 + s - 2)
    if s > 11:
        return C_FAR * (10 + s - 12)
    return C_FAR * (s - 5)


def cap_of(s):
    return C_OWN if s == 0 else (C_NEAR if s in (1, 15) else C_FAR)


def iota(shape, dim):
    return lax.broadcasted_iota(jnp.int32, shape, dim).astype(F32)


def dot_nn(a, b):
    return lax.dot_general(a, b, (((1,), (0,)), ((), ())), preferred_element_type=F32)


def dot_nt(a, b):
    return lax.dot_general(a, b, (((1,), (1,)), ((), ())), preferred_element_type=F32)


def onehot(mask):
    return jnp.where(mask, 1.0, 0.0).astype(BF16)


def col_of(row):
    eye = iota((128, 128), 0) == iota((128, 128), 1)
    return jnp.sum(jnp.where(eye, row, 0.0), axis=1, keepdims=True)


def row_of(col):
    eye = iota((128, 128), 0) == iota((128, 128), 1)
    return jnp.sum(jnp.where(eye, col, 0.0), axis=0, keepdims=True)


def norm_rows(values, gain, offset):
    center = jnp.sum(values, axis=1, keepdims=True) * (1.0 / LAT)
    centered = values - center
    spread = jnp.sum(centered * centered, axis=1, keepdims=True) * (1.0 / LAT)
    return centered * lax.rsqrt(spread + EPSILON) * gain + offset


def silu(v):
    return v / (1.0 + jnp.exp(-v))


def kernel(
    recv_i, send_i, slot, cnt, el_hbm, grid_hbm, mesh_hbm,
    w0, w1, w2, w3, w4, w5, w6,
    b0, b1, b2, b3, b4, b5, b6, b7,
    mo_hbm, eo_hbm, flag_out,
    el, grid, blk, wfull, tb, tbr, oh, tabt, t_ref, s_ref, sub_ref, r_ref, sd_ref, m_ref, rk_ref, o_ref,
    posb, posc, aq, bq, req_acc, req, reqr, m2_ref, posx,
    xc, sc, prec, metac, pre, srow, soh, serve, recvrows, scoh, msgb, mrecv, pcrow, eoc, xs, xr,
    mot, eot, mpre, mrow, vecs, flagr, flag_s,
    lsem, snd, rcv,
):
    p = lax.axis_index("patch")
    h = lax.axis_index("hidden")
    hf = h.astype(F32)
    pf = p.astype(F32)

    def hp(d):
        return lax.rem(h + d, NH)

    def pp(s):
        return lax.rem(p + s, NP)

    def remote(src, dst, ss, rs, dev):
        return pltpu.make_async_remote_copy(
            src_ref=src, dst_ref=dst, send_sem=ss, recv_sem=rs, device_id=dev, device_id_type=DEV
        )
    def got(ref, i):
        remote(ref, ref, snd.at[0], rcv.at[i], (p, h + 1 - 2 * lax.rem(h, 2))).wait_recv()

    def sent(ref, i):
        remote(ref, ref, snd.at[i], rcv.at[0], (p, h + 1 - 2 * lax.rem(h, 2))).wait_send()

    loads = [
        pltpu.make_async_copy(
            mesh_hbm.at[pl.ds(pl.multiple_of(h * SUB, SUB), SUB), :], blk, lsem.at[2]
        ),
        pltpu.make_async_copy(el_hbm, el, lsem.at[0]),
        pltpu.make_async_copy(grid_hbm, grid, lsem.at[1]),
    ]
    wsrc = (w0, w1, w2, w3, w4, w5, w6)
    wl = [pltpu.make_async_copy(wsrc[k], wfull.at[h, k], lsem.at[3]) for k in range(7)]
    for c in wl:
        c.start()
    for c in loads:
        c.start()
    barrier = pltpu.get_barrier_semaphore()
    for d in range(1, NH):
        pl.semaphore_signal(barrier, inc=1, device_id=(p, hp(d)), device_id_type=DEV)
    for s in range(1, NP):
        pl.semaphore_signal(barrier, inc=1, device_id=(pp(s), h), device_id_type=DEV)
    i128 = iota((128, 128), 0)
    i256 = iota((256, 128), 0)
    vt = slot[...].astype(F32).T
    va = jnp.floor(vt * (1.0 / 256.0))
    vb = (vt - va * 256.0).astype(BF16)
    va = (va - 256.0).astype(BF16)
    tabt[512:768, :] = jnp.zeros((256, 256), BF16)
    for k in range(3):
        n = min(256, TAB - 256 * k)
        tabt[256 * k : 256 * k + 128, 0:n] = va[:, 256 * k : 256 * k + n]
        tabt[256 * k + 128 : 256 * k + 256, 0:n] = vb[:, 256 * k : 256 * k + n]

    parity = lax.rem(h, 2)
    partner = h + 1 - 2 * parity

    def lookup(b, _):
        rr = recv_i[pl.ds(pl.multiple_of(b * 8, 8), 8), :]
        rhi = (lax.shift_right_logical(rr, 7) & 255).astype(F32)
        rtop = lax.shift_right_logical(rr, 15).astype(F32)
        rlo = (rr & 127).astype(F32)
        for k in range(8):
            oh[:, 128 * k : 128 * (k + 1)] = onehot(i256 == rhi[k : k + 1, :])
        pair = dot_nn(tabt[...], oh[...])
        for k in range(8):
            lanes = slice(128 * k, 128 * (k + 1))
            t0 = rtop[k : k + 1, :] == 0.0
            t1 = rtop[k : k + 1, :] == 1.0
            pa = jnp.where(t0, pair[0:128, lanes], jnp.where(t1, pair[256:384, lanes], pair[512:640, lanes]))
            pb = jnp.where(t0, pair[128:256, lanes], jnp.where(t1, pair[384:512, lanes], pair[640:768, lanes]))
            t_ref[pl.ds(b * 8 + k, 1), :] = jnp.sum(
                jnp.where(i128 == rlo[k : k + 1, :], (pa + 256.0) * 256.0 + pb, 0.0), axis=0, keepdims=True
            )
        return 0

    lax.fori_loop(parity * 4, parity * 4 + 4, lookup, 0)
    for k, b in enumerate((b0, b1, b2, b3, b4, b5, b6, b7)):
        tb[k : k + 1, 0:LW] = b[...]
        tb[k : k + 1, LW:128] = b[...]
    pltpu.make_async_copy(wfull.at[h], wfull.at[h], lsem.at[3]).wait()
    pl.semaphore_wait(barrier, NH - 1 + NP - 1)
    own_half = t_ref.at[pl.ds(pl.multiple_of(parity * 32, 32), 32), :]
    other_half = t_ref.at[pl.ds(pl.multiple_of(32 - parity * 32, 32), 32), :]
    swap = remote(own_half, own_half, snd.at[0], rcv.at[0], (p, partner))
    swap.start()
    t_copies = [
        remote(tb, tbr.at[h], snd.at[1], rcv.at[1], (p, hp(d))) for d in range(1, NH)
    ]
    for c in t_copies:
        c.start()
    tbr[h] = tb[...]
    ahead = 2 - 4 * parity
    w_copies = []

    def along(part, i):
        lo, n = PARTS[part]
        src_h, dst_h = ((h, h + 2), (h, h + NH - 2), (h - ahead + NH, h + ahead + NH))[i]
        ref = wfull.at[lax.rem(src_h, NH), pl.ds(lo, n)]
        return remote(ref, ref, snd.at[2], rcv.at[12 + 2 * part + i // 2], (p, lax.rem(dst_h, NH)))

    def arrived(part, i):
        lo, n = PARTS[part]
        got(wfull.at[0 : 2 - i, pl.ds(lo, n)], 12 + 2 * part + i)

    def across(part, i, base):
        lo, n = PARTS[part]
        ref = wfull.at[lax.rem(base + (0, NH - 2, 2, 4)[i], NH), pl.ds(lo, n)]
        return remote(ref, ref, snd.at[3], rcv.at[18 + part], (p, partner))

    def begin(c):
        c.start()
        w_copies.append(c)

    def stage0(part):
        begin(along(part, 0))
        begin(along(part, 1))
        begin(across(part, 0, h))

    def stage1(part):
        arrived(part, 0)
        begin(along(part, 2))
        begin(across(part, 1, h))
        begin(across(part, 2, h))

    def stage2(part):
        arrived(part, 1)
        begin(across(part, 3, h))

    def weights_ready(part):
        lo, n = PARTS[part]
        got(wfull.at[0:4, pl.ds(lo, n)], 18 + part)

    stage0(0)
    stage0(1)

    tri = jnp.where(iota((128, 256), 1) < 128.0,
                    jnp.where(iota((128, 256), 0) < iota((128, 256), 1), 1.0, 0.0), 1.0).astype(BF16)
    i16 = iota((16, 128), 0)
    base16 = jnp.zeros((16, 128), F32)
    for s in range(NP):
        base16 = jnp.where(i16 == float(s), float(base_of(s)), base16)
    cap16 = jnp.where(i16 == 0.0, float(C_OWN), jnp.where((i16 == 1.0) | (i16 == 15.0), float(C_NEAR), float(C_FAR)))
    i48 = iota((48, 128), 0)
    got(other_half, 0)
    tf = t_ref[...]
    q = jnp.floor((tf + 0.5) * (1.0 / MESH))
    rem = tf - q * MESH
    sub = jnp.floor((rem + 0.5) * (1.0 / SUB))
    r1 = rem - sub * SUB + 1.0
    shift = q - pf
    shift = jnp.where(shift < 0.0, shift + NP, shift)
    eidx = lax.broadcasted_iota(jnp.int32, (64, 128), 0) * 128 + lax.broadcasted_iota(jnp.int32, (64, 128), 1)
    live = eidx < jnp.broadcast_to(cnt[...], (64, 128))
    own = live & (sub == hf)
    s_ref[...] = jnp.where(own, shift, -1.0)
    r_ref[...] = r1
    sd_ref[...] = (send_i[...] - p * GRID).astype(F32)
    spread = jnp.where(live, sub, lax.rem(eidx, NH).astype(F32))
    sub_ref[...] = spread
    o_ref[...] = dot_nn(onehot(spread == hf), tri)

    def mark(b, _):
        st = s_ref[pl.ds(pl.multiple_of(b * 8, 8), 8), :]
        for k in range(8):
            m_ref[pl.ds(pl.multiple_of(b * 128 + 16 * k, 16), 16), :] = onehot(i16 == st[k : k + 1, :])
        return 0

    lax.fori_loop(0, 8, mark, 0)
    rk_ref[...] = dot_nn(m_ref[...], tri)
    def place(b, carry):
        counts, most = carry
        b8 = pl.ds(pl.multiple_of(b * 8, 8), 8)
        st = s_ref[b8, :]
        rt = r_ref[b8, :]
        ot = o_ref[b8, :]
        sb = sub_ref[b8, :]
        rowcount = jnp.zeros((1, 128), F32)
        pbs, pcs = [], []
        vhi = jnp.floor(rt * (1.0 / 256.0))
        vlo = rt - vhi * 256.0
        for k in range(8):
            i0 = pl.ds(pl.multiple_of(b * 128 + 16 * k, 16), 16)
            rk = rk_ref[i0, :]
            mk = m_ref[i0, :].astype(F32)
            rank = rk[:, :128] + counts
            counts = counts + rk[:, 128:]
            isown = st[k : k + 1, :] >= 0.0
            pb = jnp.sum(mk * (base16 + rank), axis=0, keepdims=True)
            rk1 = jnp.sum(mk * rank, axis=0, keepdims=True)
            pbs.append(jnp.where(isown, pb, -1.0))
            pcs.append(jnp.where(sb[k : k + 1, :] == hf, ot[k : k + 1, :128] + rowcount, -1.0))
            rowcount = rowcount + ot[k : k + 1, 128:]
            qhi0 = jnp.floor(rk1 * (1.0 / 128.0))
            qlo = rk1 - qhi0 * 128.0
            qhi = jnp.where(isown & (qhi0 < 3.0), st[k : k + 1, :] * 3.0 + qhi0, -1.0)
            hit = i48 == qhi
            lanes = pl.ds(pl.multiple_of(b * 1024 + 128 * k, 128), 128)
            aq[0:48, lanes] = jnp.where(hit, vhi[k : k + 1, :], 0.0).astype(BF16)
            aq[48:96, lanes] = jnp.where(hit, vlo[k : k + 1, :], 0.0).astype(BF16)
            bq[:, lanes] = onehot(i128 == qlo)
        for k in range(8):
            posb[pl.ds(b * 8 + k, 1), :] = pbs[k]
            posc[pl.ds(b * 8 + k, 1), :] = pcs[k]
        return counts, jnp.maximum(most, rowcount)

    counts, most = lax.fori_loop(0, 8, place, (jnp.zeros((16, 128), F32), jnp.zeros((1, 128), F32)))
    req_acc[...] = dot_nt(aq[...], bq[...])
    over = jnp.max(jnp.where(counts > cap16, 1.0, 0.0), axis=0, keepdims=True)
    over = jnp.maximum(over, jnp.where(most > float(C_BLK), 1.0, 0.0))
    for s in range(NP):
        req[s, 0:3, :] = req_acc[3 * s : 3 * s + 3, :] * 256.0 + req_acc[48 + 3 * s : 48 + 3 * s + 3, :] - 1.0
        req[s, 3:7, :] = jnp.full((4, 128), -1.0, F32)
        req[s, 7:8, :] = over
    q_copies = [
        remote(req.at[s], reqr.at[s], snd.at[4], rcv.at[2], (pp(s), h)) for s in range(1, NP)
    ]
    for c in q_copies:
        c.start()
    reqr[0] = req[0]
    for c in loads:
        c.wait()
    ic = iota((C_BLK, 128), 0)

    def compact(b, _):
        b8 = pl.ds(pl.multiple_of(b * 8, 8), 8)
        pct = posc[b8, :]
        pbt = posb[b8, :] + 1.0
        sdt = sd_ref[b8, :]
        at_b = jnp.zeros((C_BLK, 128), F32)
        at_s = jnp.zeros((C_BLK, 128), F32)
        for k in range(8):
            hit = ic == pct[k : k + 1, :]
            oh[0:C_BLK, 128 * k : 128 * (k + 1)] = onehot(hit)
            at_b = at_b + jnp.where(hit, pbt[k : k + 1, :], 0.0)
            at_s = at_s + jnp.where(hit, sdt[k : k + 1, :], 0.0)
        rows = pl.ds(pl.multiple_of(b * C_BLK, 16), C_BLK)
        xc[rows, :] = dot_nn(oh[0:C_BLK, :], el[pl.ds(pl.multiple_of(b * BLK, BLK), BLK), :]).astype(BF16)
        lanes = lax.broadcasted_iota(jnp.int32, (C_BLK, 128), 1)
        metac[rows, :] = jnp.where(
            lanes < 64,
            jnp.sum(at_b, axis=1, keepdims=True) - 1.0,
            jnp.sum(at_s, axis=1, keepdims=True),
        )
        return 0

    lax.fori_loop(0, 8, compact, 0)
    stage1(0)
    for k in range(NCOMP // 128):
        pcrow[:, 128 * k : 128 * (k + 1)] = jnp.broadcast_to(
            row_of(metac[128 * k : 128 * (k + 1), 0:1]), (8, 128)
        )

    i8 = iota((8, 128), 0)

    def mark2(b, _):
        st = sub_ref[pl.ds(pl.multiple_of(b * 8, 8), 8), :]
        for k in range(8):
            m2_ref[pl.ds(pl.multiple_of(b * 64 + 8 * k, 8), 8), :] = jnp.where(i8 == st[k : k + 1, :], 1.0, 0.0)
        return 0

    lax.fori_loop(0, 8, mark2, 0)
    rk_ref[0:512, :] = dot_nn(m2_ref[...].astype(BF16), tri)

    def place2(b, _):
        seen = jnp.zeros((8, 128), F32)
        for k in range(8):
            i0 = pl.ds(pl.multiple_of(b * 64 + 8 * k, 8), 8)
            rk = rk_ref[i0, :]
            rank = rk[:, :128] + seen
            seen = seen + rk[:, 128:]
            posx[pl.ds(b * 8 + k, 1), :] = jnp.sum(
                m2_ref[i0, :] * (i8 * float(C_BLK) + rank), axis=0, keepdims=True
            )
        return 0

    lax.fori_loop(0, 8, place2, 0)
    got(reqr.at[1:NP], 2)
    for s in range(NP):
        b, c = base_of(s), cap_of(s)
        for j in range(-(-c // 128)):
            n = min(128, c - 128 * j)
            srow[0:1, b + 128 * j : b + 128 * j + n] = reqr[s, j : j + 1, 0:n]
    flag_p = jnp.max(reqr[:, 7, :], axis=0, keepdims=True)
    flagr[h] = jnp.broadcast_to(flag_p, (8, 128))
    il640 = iota((128, SUB), 1)
    order = sum(GROUPS, ())
    ownr = slice(base_of(0), base_of(0) + C_OWN)
    g_copies = []

    def pick_rows(lo, hi):
        for k in range(lo, hi):
            soh[128 * k : 128 * (k + 1), :] = onehot(il640 == col_of(srow[0:1, 128 * k : 128 * (k + 1)]))

    ready = 0
    for gi, group in enumerate(GROUPS):
        upto = -(-(base_of(group[-1]) + cap_of(group[-1])) // 128)
        pick_rows(ready, upto)
        ready = upto
        b = base_of(group[0])
        n = sum(cap_of(s) for s in group)
        serve[b : b + n, :] = dot_nn(soh[b : b + n, :], blk[...]).astype(BF16)
        for s in group:
            rows = pl.ds(base_of(s), cap_of(s))
            c = remote(
                serve.at[rows], recvrows.at[rows], snd.at[5], rcv.at[G_SEM[gi]], (lax.rem(p + NP - s, NP), h)
            )
            c.start()
            g_copies.append(c)
    fl_copies = [
        remote(flagr.at[h], flagr.at[h], snd.at[9], rcv.at[3], (p, hp(d))) for d in range(1, NH)
    ]
    for c in fl_copies:
        c.start()
    stage1(1)
    stage0(2)
    pick_rows(ready, NROW // 128)
    recvrows[ownr, :] = dot_nn(soh[ownr, :], blk[...]).astype(BF16)
    isub = iota((SUB, 128), 0)
    for k in range(NROW // 128):
        scoh[:, 128 * k : 128 * (k + 1)] = onehot(isub == srow[0:1, 128 * k : 128 * (k + 1)])
    def gather_senders(c, _):
        rows = pl.ds(pl.multiple_of(c * SCH, 16), SCH)
        pick = metac[rows, 64:65]
        sc[rows, :] = dot_nn(onehot(iota((SCH, GRID), 1) == pick), grid[...]).astype(BF16)
        return 0

    lax.fori_loop(0, 2, gather_senders, 0)
    stage2(0)
    lax.fori_loop(2, NCOMP // SCH, gather_senders, 0)
    stage2(1)
    weights_ready(0)
    got(tbr.at[1:NH], 1)
    lane = lax.broadcasted_iota(jnp.int32, (8, 128), 1)
    for j in range(4):
        even, odd = tbr[2 * j], tbr[2 * j + 1]
        vecs[:, 128 * j : 128 * (j + 1)] = jnp.where(lane < LW, even, odd)

    def full(k):
        return wfull[:, k].reshape(LAT, LAT)

    def first(c, _):
        rows = pl.ds(pl.multiple_of(c * FCH, 16), FCH)
        prec[rows, :] = (dot_nt(xc[rows, :], full(0)) + dot_nt(sc[rows, :], full(1)) + vecs[0:1, :]).astype(BF16)
        return 0

    lax.fori_loop(0, NCOMP // FCH, first, 0)

    def arrange(c, _):
        rows = pl.ds(pl.multiple_of(c * PCH, 16), PCH)
        j0 = (c * PCH).astype(F32)
        pre[rows, :] = dot_nn(onehot(iota((PCH, NCOMP), 0) + j0 == pcrow[0:1, :]), prec[...])
        return 0

    lax.fori_loop(0, NROW // PCH, arrange, 0)

    def mlp(start, n):
        rows = slice(start, start + n)
        v = pre[rows, :] + dot_nt(recvrows[rows, :], full(2))
        hid = silu(v).astype(BF16)
        msg = norm_rows(dot_nn(hid, full(3)) + vecs[1:2, :], vecs[2:3, :], vecs[3:4, :])
        msgb[rows, :] = msg.astype(BF16)
    weights_ready(1)
    stage1(2)
    mlp(base_of(0), C_OWN // 2)
    mlp(base_of(0) + C_OWN // 2, C_OWN // 2)
    mrecv[ownr, :] = msgb[ownr, :]
    m_copies = []
    for gi, group in enumerate(GROUPS):
        start = base_of(group[0])
        n = sum(cap_of(s) for s in group)
        got(recvrows.at[start : start + n], G_SEM[gi])
        start = base_of(group[0])
        n = sum(cap_of(s) for s in group)
        for k in range(0, n, 224):
            mlp(start + k, min(224, n - k))
        for s in group:
            rows = pl.ds(base_of(s), cap_of(s))
            c = remote(msgb.at[rows], mrecv.at[rows], snd.at[6], rcv.at[7 + gi // 2], (pp(s), h))
            c.start()
            m_copies.append(c)


    def scatter_block(c, _):
        rows = pl.ds(pl.multiple_of(c * SCH, 16), SCH)
        perm = onehot(iota((SCH, NROW), 1) == metac[rows, 0:1])
        eoc[rows, :] = (xc[rows, :].astype(F32) + dot_nn(perm, msgb[...])).astype(BF16)
        return 0

    x_copies = []
    low = lax.broadcasted_iota(jnp.int32, (HALF // 2, 128), 1) < LW
    for half in range(2):
        scatter_block(jnp.int32(half), 0)
        scatter_block(jnp.int32(half + 2), 0)
        part = pl.ds(half * HALF // 2, HALF // 2)
        for j in range(4):
            cols = slice(128 * j, 128 * (j + 1))
            top = eoc[part, cols].astype(F32)
            bottom = eoc[pl.ds(HALF + half * HALF // 2, HALF // 2), cols].astype(F32)
            xs[2 * j, part, :] = jnp.where(low, top, pltpu.roll(bottom, LW, 1)).astype(BF16)
            xs[2 * j + 1, part, :] = jnp.where(low, pltpu.roll(top, LW, 1), bottom).astype(BF16)
        for d in range(1, NH):
            c = remote(xs.at[hp(d), part], xr.at[h, part], snd.at[7], rcv.at[9 + half], (p, hp(d)))
            c.start()
            x_copies.append(c)
    xr[h] = xs[h]

    lane_low = lax.broadcasted_iota(jnp.int32, (UCH, 128), 1) < LW

    def rows_arrived(half):
        got(xr.at[1:NH, pl.ds(half * HALF // 2, HALF // 2)], 9 + half)

    def edge_rows(t, _):
        b = t // (BLK // UCH)
        c = t - b * (BLK // UCH)
        x2 = xr[:, pl.ds(pl.multiple_of(b * C_BLK, 16), C_BLK), :].reshape(NCOMP, 128)
        x2 = jnp.concatenate([x2[0:HALF], x2[HALF:NCOMP]], axis=1)
        perms = []
        tops = []
        for block in (b, b + 4):
            for k in range(UCH // 128):
                col = col_of(posx[pl.ds(block * 8 + c * (UCH // 128) + k, 1), :])
                top = col >= float(HALF)
                tops.append(jnp.broadcast_to(jnp.where(top, 1.0, 0.0), (128, 128)))
                perms.append(onehot(iota((128, HALF), 1) == jnp.where(top, col - float(HALF), col)))
        got = dot_nn(jnp.concatenate(perms, axis=0), x2)
        got = jnp.where(jnp.concatenate(tops, axis=0) > 0.5, got[:, 128:256], got[:, 0:128])
        both = jnp.where(lane_low, got[0:UCH], got[UCH : 2 * UCH]).T.astype(BF16)
        eot[:, pl.ds(pl.multiple_of(b * BLK + c * UCH, 128), UCH)] = both[0:LW]
        eot[:, pl.ds(pl.multiple_of((b + 4) * BLK + c * UCH, 128), UCH)] = both[LW:128]
        return 0

    per_half = 2 * (BLK // UCH)
    stage2(2)
    got(mrecv.at[0 : base_of(1)], 7)
    first_k = 768
    for c in range(2):
        rows = slice(c * SUB // 2, (c + 1) * SUB // 2)
        mrow[rows, :] = dot_nn(scoh[rows, ownr], mrecv[ownr, :]) + dot_nn(scoh[rows, 0:first_k], mrecv[0:first_k, :])
    weights_ready(2)

    def mesh_first(c, _):
        rows = pl.ds(pl.multiple_of(c * (SUB // 2), 16), SUB // 2)
        mpre[rows, :] = dot_nt(blk[rows, :], full(4)) + vecs[4:5, :]
        return 0

    lax.fori_loop(0, 2, mesh_first, 0)
    got(mrecv.at[base_of(1) : base_of(0)], 8)
    mo_copies = []
    mo_own = []
    for i, (start, n) in enumerate(((0, 256), (256, 384))):
        rows = slice(start, start + n)
        rest = slice(first_k, base_of(0))
        total = (mrow[rows, :] + dot_nn(scoh[rows, rest], mrecv[rest, :])).astype(BF16)
        v = mpre[rows, :] + dot_nt(total, full(5))
        hid = silu(v).astype(BF16)
        upd = norm_rows(dot_nn(hid, full(6)) + vecs[5:6, :], vecs[6:7, :], vecs[7:8, :])
        mrow[rows, :] = blk[rows, :].astype(F32) + upd
        for k in range(start // 128, (start + n) // 128):
            lanes = slice(128 * k, 128 * (k + 1))
            mot[:, lanes] = mrow[lanes, :].T.astype(BF16)
        at = pl.ds(pl.multiple_of(h * SUB + start, 128), n)
        for d in range(1, NH):
            c = remote(
                mot.at[pl.ds(pl.multiple_of(hp(d) * LW, LW), LW), pl.ds(start, n)], mo_hbm.at[:, at],
                snd.at[8], rcv.at[11], (p, hp(d)),
            )
            c.start()
            mo_copies.append(c)
        c = pltpu.make_async_copy(
            mot.at[pl.ds(pl.multiple_of(h * LW, LW), LW), pl.ds(start, n)], mo_hbm.at[:, at], lsem.at[4]
        )
        c.start()
        mo_own.append(c)

    got(flagr.at[1:NH], 3)
    flag_s[0] = jnp.max(jnp.max(flagr[...], axis=0)).astype(jnp.int32)
    flag_copy = pltpu.make_async_copy(flag_s, flag_out, lsem.at[6])
    flag_copy.start()
    rows_arrived(0)
    lax.fori_loop(0, per_half, edge_rows, 0)
    rows_arrived(1)
    lax.fori_loop(per_half, 2 * per_half, edge_rows, 0)
    eo_own = pltpu.make_async_copy(eot, eo_hbm, lsem.at[5])
    eo_own.start()
    sent(own_half, 0)
    sent(tbr.at[1:NH], 1)
    sent(wfull.at[0:3], 2)
    sent(wfull.at[0:4], 3)
    sent(req.at[1:NP], 4)
    sent(serve.at[0 : base_of(0)], 5)
    sent(msgb.at[0 : base_of(0)], 6)
    sent(xs.at[1:NH], 7)
    sent(mot.at[LW:LAT], 8)
    sent(flagr.at[1:NH], 9)
    got(mo_hbm.at[:, SUB:MESH], 11)
    pltpu.make_async_copy(mot.at[0:LW], mot.at[0:LW], lsem.at[4]).wait()
    eo_own.wait()
    flag_copy.wait()


def sparse_step(grid_latent, mesh_latent, edge_latent, senders, receivers, mesh_slot, edge_counts,
                w_edge, w_sender, w_receiver, edge_bias, w_edge_out, edge_out_bias, edge_gain, edge_shift,
                w_mesh_in, w_message_in, mesh_bias, w_mesh_out, mesh_out_bias, mesh_gain, mesh_shift):
    V = pltpu.VMEM
    vm = pl.BlockSpec(memory_space=pltpu.VMEM)
    anyspec = pl.BlockSpec(memory_space=pl.ANY)
    weights = (w_edge.T, w_sender.T, w_receiver.T, w_edge_out, w_mesh_in.T, w_message_in.T, w_mesh_out)
    vectors = tuple(v.reshape(1, LW) for v in (
        edge_bias, edge_out_bias, edge_gain, edge_shift, mesh_bias, mesh_out_bias, mesh_gain, mesh_shift))
    dma = pltpu.SemaphoreType.DMA
    scratch = [
        V((EDGE, LAT), BF16), V((GRID, LAT), BF16), V((SUB, LAT), BF16), V((NH, 7, LW, LAT), BF16),
        V((8, 128), F32), V((NH, 8, 128), F32), V((256, 1024), BF16), V((768, 256), BF16), V((64, 128), F32),
        V((64, 128), F32), V((64, 128), F32), V((64, 128), F32), V((64, 128), F32),
        V((1024, 128), BF16), V((1024, 256), F32), V((64, 256), F32),
        V((64, 128), F32), V((64, 128), F32), V((96, EDGE), BF16), V((128, EDGE), BF16),
        V((96, 128), F32), V((NP, 8, 128), F32), V((NP, 8, 128), F32),
        V((512, 128), F32), V((64, 128), F32),
        V((NCOMP, LAT), BF16), V((NCOMP, LAT), BF16), V((NCOMP, LAT), BF16), V((NCOMP, 128), F32), V((NROW, LAT), F32),
        V((8, NROW), F32), V((NROW, SUB), BF16), V((NROW, LAT), BF16), V((NROW, LAT), BF16),
        V((SUB, NROW), BF16), V((NROW, LAT), BF16), V((NROW, LAT), BF16),
        V((8, NCOMP), F32), V((NCOMP, LAT), BF16), V((NH, HALF, 128), BF16), V((NH, HALF, 128), BF16),
        V((LAT, SUB), BF16), V((LW, EDGE), BF16), V((SUB, LAT), F32), V((SUB, LAT), F32), V((8, LAT), F32), V((NH, 8, 128), F32), pltpu.SMEM((1,), jnp.int32),
        dma((7,)), dma((10,)), dma((22,)),
    ]
    mo_t, eo_t, flag = pl.pallas_call(
        kernel,
        out_shape=(
            jax.ShapeDtypeStruct((LW, MESH), BF16),
            jax.ShapeDtypeStruct((LW, EDGE), BF16),
            jax.ShapeDtypeStruct((1,), jnp.int32),
        ),
        in_specs=[vm, vm, vm, vm, anyspec, anyspec, anyspec]
        + [anyspec] * 7 + [vm] * 8,
        out_specs=(anyspec, anyspec, anyspec),
        scratch_shapes=scratch,
        compiler_params=pltpu.CompilerParams(
            collective_id=0, has_side_effects=True, vmem_limit_bytes=62 * 1024 * 1024
        ),
        name="encoder",
    )(receivers.reshape(64, 128), senders.reshape(64, 128), mesh_slot.reshape(TAB, 128), edge_counts.reshape(1, 1),
      edge_latent, grid_latent, mesh_latent, *weights, *vectors)
    return mo_t, eo_t, flag


def from_everyone(x, axis):
    copies = jnp.broadcast_to(x, (lax.axis_size(axis), *x.shape))
    return lax.all_to_all(copies, axis, split_axis=0, concat_axis=0, tiled=True)


def total_of(x, axis):
    return from_everyone(x, axis).sum(axis=0)


def scatter_columns(x):
    parts = x.astype(BF16).reshape(x.shape[0], NH, LW).transpose(1, 0, 2)
    got = lax.all_to_all(parts, "hidden", split_axis=0, concat_axis=0, tiled=True)
    return got.astype(F32).sum(axis=0)


def normalize(values, gain, offset):
    center = total_of(jnp.sum(values, axis=1), "hidden") / LAT
    centered = values - center[:, None]
    spread = total_of(jnp.sum(centered * centered, axis=1), "hidden") / LAT
    return centered * lax.rsqrt(spread + EPSILON)[:, None] * gain + offset


def general_step(grid_latent, mesh_latent, edge_latent, senders, receivers, mesh_slot, edge_counts,
                 w_edge, w_sender, w_receiver, edge_bias, w_edge_out, edge_out_bias, edge_gain, edge_shift,
                 w_mesh_in, w_message_in, mesh_bias, w_mesh_out, mesh_out_bias, mesh_gain, mesh_shift):
    column = lax.axis_index("hidden")
    target = jnp.take(mesh_slot, receivers)
    sender = senders - lax.axis_index("patch") * GRID
    live = (jnp.arange(EDGE, dtype=jnp.int32) < edge_counts[0]).astype(F32)
    proj = jnp.dot(mesh_latent, w_receiver, preferred_element_type=F32).astype(BF16)
    table = from_everyone(proj, "patch").reshape(NP * MESH, LW)
    edge_pre = (
        jnp.dot(edge_latent, w_edge, preferred_element_type=F32)
        + jnp.dot(jnp.take(grid_latent, sender, axis=0), w_sender, preferred_element_type=F32)
        + jnp.take(table, target, axis=0).astype(F32)
        + edge_bias
    )
    hid = silu(edge_pre).astype(BF16)
    edge_sum = scatter_columns(jnp.dot(hid, w_edge_out, preferred_element_type=F32)) + edge_out_bias
    message = normalize(edge_sum, edge_gain, edge_shift) * live[:, None]
    cols = lax.dynamic_slice_in_dim(edge_latent, column * LW, LW, 1)
    edge_out = (cols.astype(F32) + message).astype(BF16)
    sums = jax.ops.segment_sum(message, target, num_segments=NP * MESH).astype(BF16)
    got = lax.all_to_all(sums.reshape(NP, MESH, LW), "patch", split_axis=0, concat_axis=0, tiled=True)
    own = got.astype(F32).sum(axis=0).astype(BF16)
    summed = from_everyone(own, "hidden").transpose(1, 0, 2).reshape(MESH, LAT)
    mesh_pre = (
        jnp.dot(mesh_latent, w_mesh_in, preferred_element_type=F32)
        + jnp.dot(summed, w_message_in, preferred_element_type=F32)
        + mesh_bias
    )
    hid = silu(mesh_pre).astype(BF16)
    mesh_sum = scatter_columns(jnp.dot(hid, w_mesh_out, preferred_element_type=F32)) + mesh_out_bias
    update = normalize(mesh_sum, mesh_gain, mesh_shift)
    cols = lax.dynamic_slice_in_dim(mesh_latent, column * LW, LW, 1)
    return (cols.astype(F32) + update).astype(BF16).T, edge_out.T


def step(*args):
    mo_t, eo_t, flag = sparse_step(*args)

    def again(state):
        mo, eo = general_step(*args)
        return jnp.zeros_like(state[0]), mo, eo

    mo_t, eo_t = lax.cond(flag[0] > 0, lambda: general_step(*args), lambda: (mo_t, eo_t))
    return mo_t.T, eo_t.T


def solution(mesh):
    return jax.shard_map(
        step,
        mesh=mesh,
        in_specs=(
            P("patch", None), P("patch", None), P("patch", None), P("patch"), P("patch"), P(), P("patch"),
            P(None, "hidden"), P(None, "hidden"), P(None, "hidden"), P("hidden"), P("hidden", None),
            P("hidden"), P("hidden"), P("hidden"), P(None, "hidden"), P(None, "hidden"), P("hidden"),
            P("hidden", None), P("hidden"), P("hidden"), P("hidden"),
        ),
        out_specs=(P("patch", "hidden"), P("patch", "hidden")),
        check_vma=False,
    )
```

```python
import jax
import jax.numpy as jnp
from jax import lax
from jax.experimental import pallas as pl
from jax.experimental.pallas import tpu as pltpu
from jax.sharding import PartitionSpec as P

EPSILON = 1e-05
F32 = jnp.float32
BF16 = jnp.bfloat16
NP = 16
NH = 8
LAT = 512
GRID = 3072
EDGE = 8192
MESH = 5120
SUB = MESH // NH
BLK = EDGE // NH
LW = LAT // NH
TAB = NP * MESH // 128
C_OWN, C_NEAR, C_FAR = 384, 224, 64
C_BLK = 176
NROW = C_OWN + 2 * C_NEAR + 13 * C_FAR
NCOMP = NH * C_BLK
MCH = 208
SCH = 352
EARLY = 8
FCH = 704
PCH = 416
UCH = 512
HALF = NCOMP // 2
DEV = pl.DeviceIdType.MESH
PARTS = ((0, 2), (2, 2), (4, 3))
FAR_FIRST = (4, 3, 5, 2, 6, 7, 1)
HOPS = (10, 6, 9, 11, 14, 2, 7, 8, 13, 3, 5, 12, 4, 1, 15)
GROUPS = ((5, 6, 7, 8, 9, 10, 11), (2, 3, 4, 12, 13, 14), (1,), (15,))
G_SEM = (4, 5, 6, 21)


def base_of(s):
    if s == 0:
        return NROW - C_OWN
    if s in (1, 15):
        return 13 * C_FAR + (C_NEAR if s == 15 else 0)
    if s < 5:
        return C_FAR * (7 + s - 2)
    if s > 11:
        return C_FAR * (10 + s - 12)
    return C_FAR * (s - 5)


def cap_of(s):
    return C_OWN if s == 0 else (C_NEAR if s in (1, 15) else C_FAR)


def iota(shape, dim):
    return lax.broadcasted_iota(jnp.int32, shape, dim).astype(F32)


def dot_nn(a, b):
    return lax.dot_general(a, b, (((1,), (0,)), ((), ())), preferred_element_type=F32)


def dot_nt(a, b):
    return lax.dot_general(a, b, (((1,), (1,)), ((), ())), preferred_element_type=F32)


def onehot(mask):
    return jnp.where(mask, 1.0, 0.0).astype(BF16)


def col_of(row):
    eye = iota((128, 128), 0) == iota((128, 128), 1)
    return jnp.sum(jnp.where(eye, row, 0.0), axis=1, keepdims=True)


def row_of(col):
    eye = iota((128, 128), 0) == iota((128, 128), 1)
    return jnp.sum(jnp.where(eye, col, 0.0), axis=0, keepdims=True)


def norm_rows(values, gain, offset):
    center = jnp.sum(values, axis=1, keepdims=True) * (1.0 / LAT)
    centered = values - center
    spread = jnp.sum(centered * centered, axis=1, keepdims=True) * (1.0 / LAT)
    return centered * lax.rsqrt(spread + EPSILON) * gain + offset


def silu(v):
    return v / (1.0 + jnp.exp(-v))


def kernel(
    recv_i, send_i, slot, cnt, el_hbm, grid_hbm, mesh_hbm,
    w0, w1, w2, w3, w4, w5, w6,
    b0, b1, b2, b3, b4, b5, b6, b7,
    mo_hbm, eo_hbm, flag_out,
    el, grid, blk, wfull, tb, tbr, oh, tabt, t_ref, s_ref, sub_ref, r_ref, sd_ref, m_ref, rk_ref, o_ref,
    posb, posc, aq, bq, req_acc, req, reqr, m2_ref, posx,
    xc, sc, prec, metac, pre, srow, soh, serve, recvrows, scoh, msgb, mrecv, pcrow, eoc, xs, xr,
    mot, eot, mpre, mrow, vecs, flagr, flag_s,
    lsem, snd, rcv,
):
    p = lax.axis_index("patch")
    h = lax.axis_index("hidden")
    hf = h.astype(F32)
    pf = p.astype(F32)

    def hp(d):
        return lax.rem(h + d, NH)

    def pp(s):
        return lax.rem(p + s, NP)

    def remote(src, dst, ss, rs, dev):
        return pltpu.make_async_remote_copy(
            src_ref=src, dst_ref=dst, send_sem=ss, recv_sem=rs, device_id=dev, device_id_type=DEV
        )
    def got(ref, i):
        remote(ref, ref, snd.at[0], rcv.at[i], (p, h + 1 - 2 * lax.rem(h, 2))).wait_recv()

    def sent(ref, i):
        remote(ref, ref, snd.at[i], rcv.at[0], (p, h + 1 - 2 * lax.rem(h, 2))).wait_send()

    loads = [
        pltpu.make_async_copy(
            mesh_hbm.at[pl.ds(pl.multiple_of(h * SUB, SUB), SUB), :], blk, lsem.at[2]
        ),
        pltpu.make_async_copy(el_hbm, el, lsem.at[0]),
        pltpu.make_async_copy(grid_hbm, grid, lsem.at[1]),
    ]
    wsrc = (w0, w1, w2, w3, w4, w5, w6)
    wl = [pltpu.make_async_copy(wsrc[k], wfull.at[h, k], lsem.at[3]) for k in range(7)]
    for c in wl:
        c.start()
    for c in loads:
        c.start()
    barrier = pltpu.get_barrier_semaphore()
    for d in range(1, NH):
        pl.semaphore_signal(barrier, inc=1, device_id=(p, hp(d)), device_id_type=DEV)
    for s in range(1, NP):
        pl.semaphore_signal(barrier, inc=1, device_id=(pp(s), h), device_id_type=DEV)
    i128 = iota((128, 128), 0)
    i256 = iota((256, 128), 0)
    vt = slot[...].astype(F32).T
    va = jnp.floor(vt * (1.0 / 256.0))
    vb = (vt - va * 256.0).astype(BF16)
    va = (va - 256.0).astype(BF16)
    tabt[512:768, :] = jnp.zeros((256, 256), BF16)
    for k in range(3):
        n = min(256, TAB - 256 * k)
        tabt[256 * k : 256 * k + 128, 0:n] = va[:, 256 * k : 256 * k + n]
        tabt[256 * k + 128 : 256 * k + 256, 0:n] = vb[:, 256 * k : 256 * k + n]

    parity = lax.rem(h, 2)
    partner = h + 1 - 2 * parity

    def lookup(b, _):
        rr = recv_i[pl.ds(pl.multiple_of(b * 8, 8), 8), :]
        rhi = (lax.shift_right_logical(rr, 7) & 255).astype(F32)
        rtop = lax.shift_right_logical(rr, 15).astype(F32)
        rlo = (rr & 127).astype(F32)
        for k in range(8):
            oh[:, 128 * k : 128 * (k + 1)] = onehot(i256 == rhi[k : k + 1, :])
        pair = dot_nn(tabt[...], oh[...])
        for k in range(8):
            lanes = slice(128 * k, 128 * (k + 1))
            t0 = rtop[k : k + 1, :] == 0.0
            t1 = rtop[k : k + 1, :] == 1.0
            pa = jnp.where(t0, pair[0:128, lanes], jnp.where(t1, pair[256:384, lanes], pair[512:640, lanes]))
            pb = jnp.where(t0, pair[128:256, lanes], jnp.where(t1, pair[384:512, lanes], pair[640:768, lanes]))
            t_ref[pl.ds(b * 8 + k, 1), :] = jnp.sum(
                jnp.where(i128 == rlo[k : k + 1, :], (pa + 256.0) * 256.0 + pb, 0.0), axis=0, keepdims=True
            )
        return 0

    lax.fori_loop(parity * 4, parity * 4 + 4, lookup, 0)
    for k, b in enumerate((b0, b1, b2, b3, b4, b5, b6, b7)):
        tb[k : k + 1, 0:LW] = b[...]
        tb[k : k + 1, LW:128] = b[...]
    pltpu.make_async_copy(wfull.at[h], wfull.at[h], lsem.at[3]).wait()
    pl.semaphore_wait(barrier, NH - 1 + NP - 1)
    own_half = t_ref.at[pl.ds(pl.multiple_of(parity * 32, 32), 32), :]
    other_half = t_ref.at[pl.ds(pl.multiple_of(32 - parity * 32, 32), 32), :]
    swap = remote(own_half, own_half, snd.at[0], rcv.at[0], (p, partner))
    swap.start()
    t_copies = [
        remote(tb, tbr.at[h], snd.at[1], rcv.at[1], (p, hp(d))) for d in range(1, NH)
    ]
    for c in t_copies:
        c.start()
    tbr[h] = tb[...]
    ahead = 2 - 4 * parity
    w_copies = []

    def along(part, i):
        lo, n = PARTS[part]
        src_h, dst_h = ((h, h + 2), (h, h + NH - 2), (h - ahead + NH, h + ahead + NH))[i]
        ref = wfull.at[lax.rem(src_h, NH), pl.ds(lo, n)]
        return remote(ref, ref, snd.at[2], rcv.at[12 + 2 * part + i // 2], (p, lax.rem(dst_h, NH)))

    def arrived(part, i):
        lo, n = PARTS[part]
        got(wfull.at[0 : 2 - i, pl.ds(lo, n)], 12 + 2 * part + i)

    def across(part, i, base):
        lo, n = PARTS[part]
        ref = wfull.at[lax.rem(base + (0, NH - 2, 2, 4)[i], NH), pl.ds(lo, n)]
        return remote(ref, ref, snd.at[3], rcv.at[18 + part], (p, partner))

    def begin(c):
        c.start()
        w_copies.append(c)

    def stage0(part):
        begin(along(part, 0))
        begin(along(part, 1))
        begin(across(part, 0, h))

    def stage1(part):
        arrived(part, 0)
        begin(along(part, 2))
        begin(across(part, 1, h))
        begin(across(part, 2, h))

    def stage2(part):
        arrived(part, 1)
        begin(across(part, 3, h))

    def weights_ready(part):
        lo, n = PARTS[part]
        got(wfull.at[0:4, pl.ds(lo, n)], 18 + part)

    stage0(0)
    stage0(1)

    tri = jnp.where(iota((128, 256), 1) < 128.0,
                    jnp.where(iota((128, 256), 0) < iota((128, 256), 1), 1.0, 0.0), 1.0).astype(BF16)
    i16 = iota((16, 128), 0)
    base16 = jnp.zeros((16, 128), F32)
    for s in range(NP):
        base16 = jnp.where(i16 == float(s), float(base_of(s)), base16)
    cap16 = jnp.where(i16 == 0.0, float(C_OWN), jnp.where((i16 == 1.0) | (i16 == 15.0), float(C_NEAR), float(C_FAR)))
    i48 = iota((48, 128), 0)
    got(other_half, 0)
    tf = t_ref[...]
    q = jnp.floor((tf + 0.5) * (1.0 / MESH))
    rem = tf - q * MESH
    sub = jnp.floor((rem + 0.5) * (1.0 / SUB))
    r1 = rem - sub * SUB + 1.0
    shift = q - pf
    shift = jnp.where(shift < 0.0, shift + NP, shift)
    eidx = lax.broadcasted_iota(jnp.int32, (64, 128), 0) * 128 + lax.broadcasted_iota(jnp.int32, (64, 128), 1)
    live = eidx < jnp.broadcast_to(cnt[...], (64, 128))
    own = live & (sub == hf)
    s_ref[...] = jnp.where(own, shift, -1.0)
    r_ref[...] = r1
    sd_ref[...] = (send_i[...] - p * GRID).astype(F32)
    spread = jnp.where(live, sub, lax.rem(eidx, NH).astype(F32))
    sub_ref[...] = spread
    o_ref[...] = dot_nn(onehot(spread == hf), tri)

    def mark(b, _):
        st = s_ref[pl.ds(pl.multiple_of(b * 8, 8), 8), :]
        for k in range(8):
            m_ref[pl.ds(pl.multiple_of(b * 128 + 16 * k, 16), 16), :] = onehot(i16 == st[k : k + 1, :])
        return 0

    lax.fori_loop(0, 8, mark, 0)
    rk_ref[...] = dot_nn(m_ref[...], tri)
    def place(b, carry):
        counts, most = carry
        b8 = pl.ds(pl.multiple_of(b * 8, 8), 8)
        st = s_ref[b8, :]
        rt = r_ref[b8, :]
        ot = o_ref[b8, :]
        sb = sub_ref[b8, :]
        rowcount = jnp.zeros((1, 128), F32)
        pbs, pcs = [], []
        vhi = jnp.floor(rt * (1.0 / 256.0))
        vlo = rt - vhi * 256.0
        for k in range(8):
            i0 = pl.ds(pl.multiple_of(b * 128 + 16 * k, 16), 16)
            rk = rk_ref[i0, :]
            mk = m_ref[i0, :].astype(F32)
            rank = rk[:, :128] + counts
            counts = counts + rk[:, 128:]
            isown = st[k : k + 1, :] >= 0.0
            pb = jnp.sum(mk * (base16 + rank), axis=0, keepdims=True)
            rk1 = jnp.sum(mk * rank, axis=0, keepdims=True)
            pbs.append(jnp.where(isown, pb, -1.0))
            pcs.append(jnp.where(sb[k : k + 1, :] == hf, ot[k : k + 1, :128] + rowcount, -1.0))
            rowcount = rowcount + ot[k : k + 1, 128:]
            qhi0 = jnp.floor(rk1 * (1.0 / 128.0))
            qlo = rk1 - qhi0 * 128.0
            qhi = jnp.where(isown & (qhi0 < 3.0), st[k : k + 1, :] * 3.0 + qhi0, -1.0)
            hit = i48 == qhi
            lanes = pl.ds(pl.multiple_of(b * 1024 + 128 * k, 128), 128)
            aq[0:48, lanes] = jnp.where(hit, vhi[k : k + 1, :], 0.0).astype(BF16)
            aq[48:96, lanes] = jnp.where(hit, vlo[k : k + 1, :], 0.0).astype(BF16)
            bq[:, lanes] = onehot(i128 == qlo)
        for k in range(8):
            posb[pl.ds(b * 8 + k, 1), :] = pbs[k]
            posc[pl.ds(b * 8 + k, 1), :] = pcs[k]
        return counts, jnp.maximum(most, rowcount)

    counts, most = lax.fori_loop(0, 8, place, (jnp.zeros((16, 128), F32), jnp.zeros((1, 128), F32)))
    req_acc[...] = dot_nt(aq[...], bq[...])
    over = jnp.max(jnp.where(counts > cap16, 1.0, 0.0), axis=0, keepdims=True)
    over = jnp.maximum(over, jnp.where(most > float(C_BLK), 1.0, 0.0))
    for s in range(NP):
        req[s, 0:3, :] = req_acc[3 * s : 3 * s + 3, :] * 256.0 + req_acc[48 + 3 * s : 48 + 3 * s + 3, :] - 1.0
        req[s, 3:7, :] = jnp.full((4, 128), -1.0, F32)
        req[s, 7:8, :] = over
    q_copies = [
        remote(req.at[s], reqr.at[s], snd.at[4], rcv.at[2], (pp(s), h)) for s in range(1, NP)
    ]
    for c in q_copies:
        c.start()
    reqr[0] = req[0]
    for c in loads:
        c.wait()
    ic = iota((C_BLK, 128), 0)

    def compact(b, _):
        b8 = pl.ds(pl.multiple_of(b * 8, 8), 8)
        pct = posc[b8, :]
        pbt = posb[b8, :] + 1.0
        sdt = sd_ref[b8, :]
        at_b = jnp.zeros((C_BLK, 128), F32)
        at_s = jnp.zeros((C_BLK, 128), F32)
        for k in range(8):
            hit = ic == pct[k : k + 1, :]
            oh[0:C_BLK, 128 * k : 128 * (k + 1)] = onehot(hit)
            at_b = at_b + jnp.where(hit, pbt[k : k + 1, :], 0.0)
            at_s = at_s + jnp.where(hit, sdt[k : k + 1, :], 0.0)
        rows = pl.ds(pl.multiple_of(b * C_BLK, 16), C_BLK)
        xc[rows, :] = dot_nn(oh[0:C_BLK, :], el[pl.ds(pl.multiple_of(b * BLK, BLK), BLK), :]).astype(BF16)
        lanes = lax.broadcasted_iota(jnp.int32, (C_BLK, 128), 1)
        metac[rows, :] = jnp.where(
            lanes < 64,
            jnp.sum(at_b, axis=1, keepdims=True) - 1.0,
            jnp.sum(at_s, axis=1, keepdims=True),
        )
        return 0

    lax.fori_loop(0, 8, compact, 0)
    stage1(0)
    for k in range(NCOMP // 128):
        pcrow[:, 128 * k : 128 * (k + 1)] = jnp.broadcast_to(
            row_of(metac[128 * k : 128 * (k + 1), 0:1]), (8, 128)
        )

    i8 = iota((8, 128), 0)

    def mark2(b, _):
        st = sub_ref[pl.ds(pl.multiple_of(b * 8, 8), 8), :]
        for k in range(8):
            m2_ref[pl.ds(pl.multiple_of(b * 64 + 8 * k, 8), 8), :] = jnp.where(i8 == st[k : k + 1, :], 1.0, 0.0)
        return 0

    lax.fori_loop(0, 8, mark2, 0)
    rk_ref[0:512, :] = dot_nn(m2_ref[...].astype(BF16), tri)

    def place2(b, _):
        seen = jnp.zeros((8, 128), F32)
        for k in range(8):
            i0 = pl.ds(pl.multiple_of(b * 64 + 8 * k, 8), 8)
            rk = rk_ref[i0, :]
            rank = rk[:, :128] + seen
            seen = seen + rk[:, 128:]
            posx[pl.ds(b * 8 + k, 1), :] = jnp.sum(
                m2_ref[i0, :] * (i8 * float(C_BLK) + rank), axis=0, keepdims=True
            )
        return 0

    lax.fori_loop(0, 8, place2, 0)
    got(reqr.at[1:NP], 2)
    for s in range(NP):
        b, c = base_of(s), cap_of(s)
        for j in range(-(-c // 128)):
            n = min(128, c - 128 * j)
            srow[0:1, b + 128 * j : b + 128 * j + n] = reqr[s, j : j + 1, 0:n]
    flag_p = jnp.max(reqr[:, 7, :], axis=0, keepdims=True)
    flagr[h] = jnp.broadcast_to(flag_p, (8, 128))
    il640 = iota((128, SUB), 1)
    order = sum(GROUPS, ())
    ownr = slice(base_of(0), base_of(0) + C_OWN)
    g_copies = []

    def pick_rows(lo, hi):
        for k in range(lo, hi):
            soh[128 * k : 128 * (k + 1), :] = onehot(il640 == col_of(srow[0:1, 128 * k : 128 * (k + 1)]))

    ready = 0
    for gi, group in enumerate(GROUPS):
        upto = -(-(base_of(group[-1]) + cap_of(group[-1])) // 128)
        pick_rows(ready, upto)
        ready = upto
        b = base_of(group[0])
        n = sum(cap_of(s) for s in group)
        serve[b : b + n, :] = dot_nn(soh[b : b + n, :], blk[...]).astype(BF16)
        for s in sorted(group, key=HOPS.index):
            rows = pl.ds(base_of(s), cap_of(s))
            c = remote(
                serve.at[rows], recvrows.at[rows], snd.at[5], rcv.at[G_SEM[gi]], (lax.rem(p + NP - s, NP), h)
            )
            c.start()
            g_copies.append(c)
    fl_copies = [
        remote(flagr.at[h], flagr.at[h], snd.at[9], rcv.at[3], (p, hp(d))) for d in range(1, NH)
    ]
    for c in fl_copies:
        c.start()
    stage1(1)
    stage0(2)
    pick_rows(ready, NROW // 128)
    recvrows[ownr, :] = dot_nn(soh[ownr, :], blk[...]).astype(BF16)
    isub = iota((SUB, 128), 0)
    for k in range(NROW // 128):
        scoh[:, 128 * k : 128 * (k + 1)] = onehot(isub == srow[0:1, 128 * k : 128 * (k + 1)])
    def gather_senders(c, _):
        rows = pl.ds(pl.multiple_of(c * SCH, 16), SCH)
        pick = metac[rows, 64:65]
        sc[rows, :] = dot_nn(onehot(iota((SCH, GRID), 1) == pick), grid[...]).astype(BF16)
        return 0

    lax.fori_loop(0, 2, gather_senders, 0)
    stage2(0)
    lax.fori_loop(2, NCOMP // SCH, gather_senders, 0)
    stage2(1)
    weights_ready(0)
    got(tbr.at[1:NH], 1)
    lane = lax.broadcasted_iota(jnp.int32, (8, 128), 1)
    for j in range(4):
        even, odd = tbr[2 * j], tbr[2 * j + 1]
        vecs[:, 128 * j : 128 * (j + 1)] = jnp.where(lane < LW, even, odd)

    def full(k):
        return wfull[:, k].reshape(LAT, LAT)

    def first(c, _):
        rows = pl.ds(pl.multiple_of(c * FCH, 16), FCH)
        prec[rows, :] = (dot_nt(xc[rows, :], full(0)) + dot_nt(sc[rows, :], full(1)) + vecs[0:1, :]).astype(BF16)
        return 0

    lax.fori_loop(0, NCOMP // FCH, first, 0)

    def arrange(c, _):
        rows = pl.ds(pl.multiple_of(c * PCH, 16), PCH)
        j0 = (c * PCH).astype(F32)
        pre[rows, :] = dot_nn(onehot(iota((PCH, NCOMP), 0) + j0 == pcrow[0:1, :]), prec[...])
        return 0

    lax.fori_loop(0, NROW // PCH, arrange, 0)

    def mlp(start, n):
        rows = slice(start, start + n)
        v = pre[rows, :] + dot_nt(recvrows[rows, :], full(2))
        hid = silu(v).astype(BF16)
        msg = norm_rows(dot_nn(hid, full(3)) + vecs[1:2, :], vecs[2:3, :], vecs[3:4, :])
        msgb[rows, :] = msg.astype(BF16)
    weights_ready(1)
    stage1(2)
    mlp(base_of(0), C_OWN // 2)
    mlp(base_of(0) + C_OWN // 2, C_OWN // 2)
    mrecv[ownr, :] = msgb[ownr, :]
    m_copies = []
    for gi, group in enumerate(GROUPS):
        start = base_of(group[0])
        n = sum(cap_of(s) for s in group)
        got(recvrows.at[start : start + n], G_SEM[gi])
        start = base_of(group[0])
        n = sum(cap_of(s) for s in group)
        for k in range(0, n, 224):
            mlp(start + k, min(224, n - k))
        for s in sorted(group, key=HOPS.index):
            rows = pl.ds(base_of(s), cap_of(s))
            c = remote(msgb.at[rows], mrecv.at[rows], snd.at[6], rcv.at[7 + gi // 2], (pp(s), h))
            c.start()
            m_copies.append(c)


    def scatter_block(c, _):
        rows = pl.ds(pl.multiple_of(c * SCH, 16), SCH)
        perm = onehot(iota((SCH, NROW), 1) == metac[rows, 0:1])
        eoc[rows, :] = (xc[rows, :].astype(F32) + dot_nn(perm, msgb[...])).astype(BF16)
        return 0

    x_copies = []
    low = lax.broadcasted_iota(jnp.int32, (HALF // 2, 128), 1) < LW
    for half in range(2):
        scatter_block(jnp.int32(half), 0)
        scatter_block(jnp.int32(half + 2), 0)
        part = pl.ds(half * HALF // 2, HALF // 2)
        for j in range(4):
            cols = slice(128 * j, 128 * (j + 1))
            top = eoc[part, cols].astype(F32)
            bottom = eoc[pl.ds(HALF + half * HALF // 2, HALF // 2), cols].astype(F32)
            xs[2 * j, part, :] = jnp.where(low, top, pltpu.roll(bottom, LW, 1)).astype(BF16)
            xs[2 * j + 1, part, :] = jnp.where(low, pltpu.roll(top, LW, 1), bottom).astype(BF16)
        for d in FAR_FIRST:
            c = remote(xs.at[hp(d), part], xr.at[h, part], snd.at[7], rcv.at[9 + half], (p, hp(d)))
            c.start()
            x_copies.append(c)
    xr[h] = xs[h]

    lane_low = lax.broadcasted_iota(jnp.int32, (UCH, 128), 1) < LW

    def rows_arrived(half):
        got(xr.at[1:NH, pl.ds(half * HALF // 2, HALF // 2)], 9 + half)

    def edge_rows(t, _):
        b = t // (BLK // UCH)
        c = t - b * (BLK // UCH)
        x2 = xr[:, pl.ds(pl.multiple_of(b * C_BLK, 16), C_BLK), :].reshape(NCOMP, 128)
        x2 = jnp.concatenate([x2[0:HALF], x2[HALF:NCOMP]], axis=1)
        perms = []
        tops = []
        for block in (b, b + 4):
            for k in range(UCH // 128):
                col = col_of(posx[pl.ds(block * 8 + c * (UCH // 128) + k, 1), :])
                top = col >= float(HALF)
                tops.append(jnp.broadcast_to(jnp.where(top, 1.0, 0.0), (128, 128)))
                perms.append(onehot(iota((128, HALF), 1) == jnp.where(top, col - float(HALF), col)))
        got = dot_nn(jnp.concatenate(perms, axis=0), x2)
        got = jnp.where(jnp.concatenate(tops, axis=0) > 0.5, got[:, 128:256], got[:, 0:128])
        both = jnp.where(lane_low, got[0:UCH], got[UCH : 2 * UCH]).T.astype(BF16)
        eot[:, pl.ds(pl.multiple_of(b * BLK + c * UCH, 128), UCH)] = both[0:LW]
        eot[:, pl.ds(pl.multiple_of((b + 4) * BLK + c * UCH, 128), UCH)] = both[LW:128]
        return 0

    per_half = 2 * (BLK // UCH)
    stage2(2)
    got(mrecv.at[0 : base_of(1)], 7)
    first_k = 768
    for c in range(2):
        rows = slice(c * SUB // 2, (c + 1) * SUB // 2)
        mrow[rows, :] = dot_nn(scoh[rows, ownr], mrecv[ownr, :]) + dot_nn(scoh[rows, 0:first_k], mrecv[0:first_k, :])
    weights_ready(2)

    def mesh_first(c, _):
        rows = pl.ds(pl.multiple_of(c * (SUB // 2), 16), SUB // 2)
        mpre[rows, :] = dot_nt(blk[rows, :], full(4)) + vecs[4:5, :]
        return 0

    lax.fori_loop(0, 2, mesh_first, 0)
    got(mrecv.at[base_of(1) : base_of(0)], 8)
    mo_copies = []
    mo_own = []
    for i, (start, n) in enumerate(((0, 256), (256, 384))):
        rows = slice(start, start + n)
        rest = slice(first_k, base_of(0))
        total = (mrow[rows, :] + dot_nn(scoh[rows, rest], mrecv[rest, :])).astype(BF16)
        v = mpre[rows, :] + dot_nt(total, full(5))
        hid = silu(v).astype(BF16)
        upd = norm_rows(dot_nn(hid, full(6)) + vecs[5:6, :], vecs[6:7, :], vecs[7:8, :])
        mrow[rows, :] = blk[rows, :].astype(F32) + upd
        for k in range(start // 128, (start + n) // 128):
            lanes = slice(128 * k, 128 * (k + 1))
            mot[:, lanes] = mrow[lanes, :].T.astype(BF16)
        at = pl.ds(pl.multiple_of(h * SUB + start, 128), n)
        for d in FAR_FIRST:
            c = remote(
                mot.at[pl.ds(pl.multiple_of(hp(d) * LW, LW), LW), pl.ds(start, n)], mo_hbm.at[:, at],
                snd.at[8], rcv.at[11], (p, hp(d)),
            )
            c.start()
            mo_copies.append(c)
        c = pltpu.make_async_copy(
            mot.at[pl.ds(pl.multiple_of(h * LW, LW), LW), pl.ds(start, n)], mo_hbm.at[:, at], lsem.at[4]
        )
        c.start()
        mo_own.append(c)

    got(flagr.at[1:NH], 3)
    flag_s[0] = jnp.max(jnp.max(flagr[...], axis=0)).astype(jnp.int32)
    flag_copy = pltpu.make_async_copy(flag_s, flag_out, lsem.at[6])
    flag_copy.start()
    rows_arrived(0)
    lax.fori_loop(0, per_half, edge_rows, 0)
    rows_arrived(1)
    lax.fori_loop(per_half, 2 * per_half, edge_rows, 0)
    eo_own = pltpu.make_async_copy(eot, eo_hbm, lsem.at[5])
    eo_own.start()
    sent(own_half, 0)
    sent(tbr.at[1:NH], 1)
    sent(wfull.at[0:3], 2)
    sent(wfull.at[0:4], 3)
    sent(req.at[1:NP], 4)
    sent(serve.at[0 : base_of(0)], 5)
    sent(msgb.at[0 : base_of(0)], 6)
    sent(xs.at[1:NH], 7)
    sent(mot.at[LW:LAT], 8)
    sent(flagr.at[1:NH], 9)
    got(mo_hbm.at[:, SUB:MESH], 11)
    pltpu.make_async_copy(mot.at[0:LW], mot.at[0:LW], lsem.at[4]).wait()
    eo_own.wait()
    flag_copy.wait()


def sparse_step(grid_latent, mesh_latent, edge_latent, senders, receivers, mesh_slot, edge_counts,
                w_edge, w_sender, w_receiver, edge_bias, w_edge_out, edge_out_bias, edge_gain, edge_shift,
                w_mesh_in, w_message_in, mesh_bias, w_mesh_out, mesh_out_bias, mesh_gain, mesh_shift):
    V = pltpu.VMEM
    vm = pl.BlockSpec(memory_space=pltpu.VMEM)
    anyspec = pl.BlockSpec(memory_space=pl.ANY)
    weights = (w_edge.T, w_sender.T, w_receiver.T, w_edge_out, w_mesh_in.T, w_message_in.T, w_mesh_out)
    vectors = tuple(v.reshape(1, LW) for v in (
        edge_bias, edge_out_bias, edge_gain, edge_shift, mesh_bias, mesh_out_bias, mesh_gain, mesh_shift))
    dma = pltpu.SemaphoreType.DMA
    scratch = [
        V((EDGE, LAT), BF16), V((GRID, LAT), BF16), V((SUB, LAT), BF16), V((NH, 7, LW, LAT), BF16),
        V((8, 128), F32), V((NH, 8, 128), F32), V((256, 1024), BF16), V((768, 256), BF16), V((64, 128), F32),
        V((64, 128), F32), V((64, 128), F32), V((64, 128), F32), V((64, 128), F32),
        V((1024, 128), BF16), V((1024, 256), F32), V((64, 256), F32),
        V((64, 128), F32), V((64, 128), F32), V((96, EDGE), BF16), V((128, EDGE), BF16),
        V((96, 128), F32), V((NP, 8, 128), F32), V((NP, 8, 128), F32),
        V((512, 128), F32), V((64, 128), F32),
        V((NCOMP, LAT), BF16), V((NCOMP, LAT), BF16), V((NCOMP, LAT), BF16), V((NCOMP, 128), F32), V((NROW, LAT), F32),
        V((8, NROW), F32), V((NROW, SUB), BF16), V((NROW, LAT), BF16), V((NROW, LAT), BF16),
        V((SUB, NROW), BF16), V((NROW, LAT), BF16), V((NROW, LAT), BF16),
        V((8, NCOMP), F32), V((NCOMP, LAT), BF16), V((NH, HALF, 128), BF16), V((NH, HALF, 128), BF16),
        V((LAT, SUB), BF16), V((LW, EDGE), BF16), V((SUB, LAT), F32), V((SUB, LAT), F32), V((8, LAT), F32), V((NH, 8, 128), F32), pltpu.SMEM((1,), jnp.int32),
        dma((7,)), dma((10,)), dma((22,)),
    ]
    mo_t, eo_t, flag = pl.pallas_call(
        kernel,
        out_shape=(
            jax.ShapeDtypeStruct((LW, MESH), BF16),
            jax.ShapeDtypeStruct((LW, EDGE), BF16),
            jax.ShapeDtypeStruct((1,), jnp.int32),
        ),
        in_specs=[vm, vm, vm, vm, anyspec, anyspec, anyspec]
        + [anyspec] * 7 + [vm] * 8,
        out_specs=(anyspec, anyspec, anyspec),
        scratch_shapes=scratch,
        compiler_params=pltpu.CompilerParams(
            collective_id=0, has_side_effects=True, vmem_limit_bytes=62 * 1024 * 1024
        ),
        name="encoder",
    )(receivers.reshape(64, 128), senders.reshape(64, 128), mesh_slot.reshape(TAB, 128), edge_counts.reshape(1, 1),
      edge_latent, grid_latent, mesh_latent, *weights, *vectors)
    return mo_t, eo_t, flag


def from_everyone(x, axis):
    copies = jnp.broadcast_to(x, (lax.axis_size(axis), *x.shape))
    return lax.all_to_all(copies, axis, split_axis=0, concat_axis=0, tiled=True)


def total_of(x, axis):
    return from_everyone(x, axis).sum(axis=0)


def scatter_columns(x):
    parts = x.astype(BF16).reshape(x.shape[0], NH, LW).transpose(1, 0, 2)
    got = lax.all_to_all(parts, "hidden", split_axis=0, concat_axis=0, tiled=True)
    return got.astype(F32).sum(axis=0)


def normalize(values, gain, offset):
    center = total_of(jnp.sum(values, axis=1), "hidden") / LAT
    centered = values - center[:, None]
    spread = total_of(jnp.sum(centered * centered, axis=1), "hidden") / LAT
    return centered * lax.rsqrt(spread + EPSILON)[:, None] * gain + offset


def general_step(grid_latent, mesh_latent, edge_latent, senders, receivers, mesh_slot, edge_counts,
                 w_edge, w_sender, w_receiver, edge_bias, w_edge_out, edge_out_bias, edge_gain, edge_shift,
                 w_mesh_in, w_message_in, mesh_bias, w_mesh_out, mesh_out_bias, mesh_gain, mesh_shift):
    column = lax.axis_index("hidden")
    target = jnp.take(mesh_slot, receivers)
    sender = senders - lax.axis_index("patch") * GRID
    live = (jnp.arange(EDGE, dtype=jnp.int32) < edge_counts[0]).astype(F32)
    proj = jnp.dot(mesh_latent, w_receiver, preferred_element_type=F32).astype(BF16)
    table = from_everyone(proj, "patch").reshape(NP * MESH, LW)
    edge_pre = (
        jnp.dot(edge_latent, w_edge, preferred_element_type=F32)
        + jnp.dot(jnp.take(grid_latent, sender, axis=0), w_sender, preferred_element_type=F32)
        + jnp.take(table, target, axis=0).astype(F32)
        + edge_bias
    )
    hid = silu(edge_pre).astype(BF16)
    edge_sum = scatter_columns(jnp.dot(hid, w_edge_out, preferred_element_type=F32)) + edge_out_bias
    message = normalize(edge_sum, edge_gain, edge_shift) * live[:, None]
    cols = lax.dynamic_slice_in_dim(edge_latent, column * LW, LW, 1)
    edge_out = (cols.astype(F32) + message).astype(BF16)
    sums = jax.ops.segment_sum(message, target, num_segments=NP * MESH).astype(BF16)
    got = lax.all_to_all(sums.reshape(NP, MESH, LW), "patch", split_axis=0, concat_axis=0, tiled=True)
    own = got.astype(F32).sum(axis=0).astype(BF16)
    summed = from_everyone(own, "hidden").transpose(1, 0, 2).reshape(MESH, LAT)
    mesh_pre = (
        jnp.dot(mesh_latent, w_mesh_in, preferred_element_type=F32)
        + jnp.dot(summed, w_message_in, preferred_element_type=F32)
        + mesh_bias
    )
    hid = silu(mesh_pre).astype(BF16)
    mesh_sum = scatter_columns(jnp.dot(hid, w_mesh_out, preferred_element_type=F32)) + mesh_out_bias
    update = normalize(mesh_sum, mesh_gain, mesh_shift)
    cols = lax.dynamic_slice_in_dim(mesh_latent, column * LW, LW, 1)
    return (cols.astype(F32) + update).astype(BF16).T, edge_out.T


def step(*args):
    mo_t, eo_t, flag = sparse_step(*args)

    def again(state):
        mo, eo = general_step(*args)
        return jnp.zeros_like(state[0]), mo, eo

    mo_t, eo_t = lax.cond(flag[0] > 0, lambda: general_step(*args), lambda: (mo_t, eo_t))
    return mo_t.T, eo_t.T


def solution(mesh):
    return jax.shard_map(
        step,
        mesh=mesh,
        in_specs=(
            P("patch", None), P("patch", None), P("patch", None), P("patch"), P("patch"), P(), P("patch"),
            P(None, "hidden"), P(None, "hidden"), P(None, "hidden"), P("hidden"), P("hidden", None),
            P("hidden"), P("hidden"), P("hidden"), P(None, "hidden"), P(None, "hidden"), P("hidden"),
            P("hidden", None), P("hidden"), P("hidden"), P("hidden"),
        ),
        out_specs=(P("patch", "hidden"), P("patch", "hidden")),
        check_vma=False,
    )
```
